32 devices in a mesh: gx: 2 (over core), gy: 4 (over y, x), gz: 4 (over z).
Axes of the slice: x: 2, y: 2, z: 4, core: 2. Of those that a mesh axis runs over, the one named last changes fastest.
Arguments:
- block_values: bfloat16 [4, 64, 4, 6, 128, 128], P('gy', 'gx', 'gz'), as said below
- block_cols: int32 [4, 64, 4, 6], P('gy', 'gx', 'gz'), may hold values from 0 to 63, as said below
Outputs:
- purified: float32 [256, 32768], P(('gx', 'gy'), 'gz')
The draws below stay inside these ranges and needn't reach their ends.
Inputs may be any that keep to these rules, and one draw needn't show every extreme that they name: block_cols[a, s, b, :] holds 6 distinct tile columns of panel b at which tile row a * 64 + s of P is nonzero; every tile column of a panel is listed by exactly 6 tile rows of each slab; the pattern is symmetric: tile (i, j) is listed exactly when tile (j, i) is. `block_values`: P is symmetric: the tile listed at (i, j) is the transpose of the tile listed at (j, i), and diagonal tiles are symmetric.
All inputs are finite; a program needn't handle non-finite values.
Results may differ from the reference program's by a relative error of at most 0.0033.
Values may be sent and summed in bfloat16 or wider, within the bound.
No kernel may reach another device: no remote copies, remote signals or barrier semaphores. Data moves between devices by JAX's collectives and lax.ppermute only.
A program may use at most 128 MiB of HBM per device.

```python
import jax
import jax.numpy as jnp
from jax import lax

TILE = 128
NT = 256
KP = 6
WIN = 1
NPAN = 4
ST = 64
RB = 32
ORDER = 32768
N_GX = 2


def tile_pattern(key):
    pattern_key = jax.random.fold_in(key, 11)
    split_keys = jax.random.split(pattern_key, 2)
    order_keys = jax.random.split(split_keys[0], NPAN * NPAN * 2)
    orders = jax.vmap(lambda subkey: jax.random.permutation(subkey, ST))(order_keys).reshape(NPAN, NPAN, 2, ST)
    first = orders[:, :, 0].astype(jnp.int32)
    second = orders[:, :, 1].astype(jnp.int32)
    slab_index = jnp.arange(NPAN, dtype=jnp.int32)[:, None, None]
    panel_index = jnp.arange(NPAN, dtype=jnp.int32)[None, :, None]
    lower_part = slab_index > panel_index
    on_diagonal = slab_index == panel_index
    first_swapped = jnp.swapaxes(first, 0, 1)
    second_swapped = jnp.swapaxes(second, 0, 1)
    source_order = jnp.where(lower_part, second_swapped, first)
    target_order = jnp.where(lower_part, first_swapped, jnp.where(on_diagonal, first, second))
    target_inverse = jnp.argsort(target_order, axis=-1).astype(jnp.int32)
    extra_shifts = (jax.random.permutation(split_keys[1], ST // 2 - 1)[:(KP - 2) // 2] + 1).astype(jnp.int32)
    shifts = jnp.concatenate([jnp.array([0, ST // 2], jnp.int32), extra_shifts, -extra_shifts])
    position = (source_order[:, :, :, None] + shifts[None, None, None, :]) % ST
    columns = jnp.take_along_axis(target_inverse, position.reshape(NPAN, NPAN, ST * KP), axis=2)
    return jnp.transpose(columns.reshape(NPAN, NPAN, ST, KP), (0, 2, 1, 3)).astype(jnp.int32)


def draw_block_cols(key, part):
    return tile_pattern(key)


def draw_block_values(key, part):
    columns = tile_pattern(key)
    row_global = jnp.broadcast_to((jnp.arange(NPAN, dtype=jnp.int32)[:, None] * ST + jnp.arange(ST, dtype=jnp.int32)[None, :])[:, :, None, None], (NPAN, ST, NPAN, KP))
    col_global = jnp.arange(NPAN, dtype=jnp.int32)[None, None, :, None] * ST + columns
    tile_ident = (jnp.minimum(row_global, col_global) * NT + jnp.maximum(row_global, col_global)).reshape(-1)
    value_key = jax.random.fold_in(key, 23)

    def one_tile(ident):
        subkey = jax.random.fold_in(value_key, ident)
        return jax.random.normal(subkey, (TILE, TILE), jnp.float32)
    raw_tiles = jax.vmap(one_tile)(tile_ident)
    flipped = (row_global > col_global).reshape(-1)[:, None, None]
    diagonal_mask = (row_global == col_global).reshape(-1)[:, None, None]
    swapped = jnp.swapaxes(raw_tiles, 1, 2)
    tiles = jnp.where(flipped, swapped, raw_tiles)
    tiles = jnp.where(diagonal_mask, (raw_tiles + swapped) * 0.7071, tiles)
    scale = 2.0 / (NPAN * KP * TILE) ** 0.5
    return (tiles * scale).reshape(NPAN, ST, NPAN, KP, TILE, TILE).astype(jnp.bfloat16)


def setup_inputs(seed: int = 0) -> dict:
    splits = jax.random.split(jax.random.key(seed), 3)
    return {
        "block_values": draw_block_values(jax.random.fold_in(splits[2], 71), 0),
        "block_cols": draw_block_cols(jax.random.fold_in(splits[2], 71), 0),
    }


def dense_rows(row_tiles, row_columns):
    count_rows = row_tiles.shape[0]
    global_cols = (jnp.arange(NPAN, dtype=jnp.int32)[None, :, None] * ST + row_columns).reshape(count_rows, NPAN * KP)
    onehot = (global_cols[:, :, None] == jnp.arange(NT, dtype=jnp.int32)[None, None, :]).astype(jnp.float32)
    flattened = row_tiles.reshape(count_rows, NPAN * KP, TILE, TILE).astype(jnp.float32)
    densified = jnp.einsum("nqj,nqyx->nyjx", onehot, flattened)
    return densified.reshape(count_rows * TILE, ORDER)


def times_matrix(left_rows, block_values, block_cols):
    height = left_rows.shape[0]
    all_tiles = block_values.reshape(NT, NPAN * KP, TILE, TILE)
    all_columns = (jnp.arange(NPAN, dtype=jnp.int32)[None, :, None] * ST + block_cols.reshape(NT, NPAN, KP)).reshape(NT, NPAN * KP)

    def advance(running, inputs):
        row_tiles, row_columns, tile_row = inputs
        portion = lax.dynamic_slice_in_dim(left_rows, tile_row * TILE, TILE, 1)
        product = jnp.einsum("rx,qxy->rqy", portion, row_tiles.astype(jnp.float32))
        return running.at[:, row_columns, :].add(product), None

    running = jnp.zeros((height, NT, TILE), jnp.float32)
    running, ignored = lax.scan(advance, running, (all_tiles, all_columns, jnp.arange(NT, dtype=jnp.int32)))
    return running.reshape(height, ORDER)


def reference(block_values, block_cols):
    window_index = (jnp.arange(N_GX, dtype=jnp.int32)[:, None] * RB + jnp.arange(WIN, dtype=jnp.int32)[None, :]).reshape(-1)
    left_rows = dense_rows(block_values[0][window_index], block_cols[0][window_index])
    square = times_matrix(left_rows, block_values, block_cols)
    rounded = lax.optimization_barrier(square.astype(jnp.bfloat16)).astype(jnp.float32)
    return 3.0 * square - 2.0 * times_matrix(rounded, block_values, block_cols)
```

```python
import functools

import jax
import jax.numpy as jnp
from jax import lax
from jax.experimental import pallas as pl
from jax.experimental.pallas import tpu as pltpu
from jax.sharding import PartitionSpec as P

WIN = 1
VMEM = pltpu.MemorySpace.VMEM
SMEM = pltpu.MemorySpace.SMEM


def swaps(size, step):
    return [(i, i ^ step) for i in range(size)]


def invert_kernel(cols_ref, inv_ref, count_ref):
    rows, slots = cols_ref.shape

    @pl.loop(0, rows)
    def _(y):
        count_ref[y] = 0

    @pl.loop(0, rows)
    def _(p):
        for j in range(slots):
            y = cols_ref[p, j]
            n = count_ref[y]
            inv_ref[y, n] = p * 8 + j
            count_ref[y] = n + 1


def invert(columns):
    return pl.pallas_call(
        invert_kernel,
        out_shape=jax.ShapeDtypeStruct(columns.shape, jnp.int32),
        in_specs=[pl.BlockSpec(memory_space=SMEM)],
        out_specs=pl.BlockSpec(memory_space=SMEM),
        scratch_shapes=[pltpu.SMEM((columns.shape[0],), jnp.int32)],
        cost_estimate=pl.CostEstimate(flops=4_000_000, bytes_accessed=4096, transcendentals=0),
        name="invert",
    )(columns)


def product_one_kernel(by_rows, parts, lefts, index_ref, *refs):
    left_refs, refs = refs[:lefts], refs[lefts:]
    part_refs, refs = refs[:parts], refs[parts:]
    blocks = len(refs) - 4
    send_refs, (left_ref, tile_ref, acc_ref, sems) = refs[:blocks], refs[blocks:]
    g, a, b = lax.axis_index("gx"), lax.axis_index("gy"), lax.axis_index("gz")
    here = part_refs[0].shape[0]
    slab = here * parts
    slots = tile_ref.shape[0]
    height = acc_ref.shape[0] * acc_ref.shape[2]
    chosen = a ^ b if by_rows else a
    for k in range(lefts):

        @pl.when(chosen == k)
        def _(k=k):
            left_ref[...] = left_refs[k][...]

    tail = left_ref[pl.ds(slots * height, 16), :].astype(jnp.float32)
    targets = []
    for k in range(slots):
        column = jnp.max(tail[k : k + 1, :]).astype(jnp.int32)
        if by_rows:
            p = lax.rem(column + slab - here * g, slab)
            row = lax.rem(p, here)
            for t in range(parts):

                @pl.when(p // here == t)
                def _(k=k, t=t, row=row):
                    pltpu.make_async_copy(part_refs[t].at[row], tile_ref.at[k], sems.at[k, 0]).start()

            targets.append([index_ref[p, j] for j in range(slots)])
        else:
            targets.append([])
            for n in range(slots):
                entry = index_ref[column, n]
                p, j = entry >> 3, entry & 7
                row = lax.rem(p, here)
                for t in range(parts):

                    @pl.when(p // here == t)
                    def _(k=k, n=n, t=t, row=row, j=j):
                        pltpu.make_async_copy(
                            part_refs[t].at[row, j], tile_ref.at[k, n], sems.at[k, n]
                        ).start()

                targets[k].append(p)
    acc_ref[...] = jnp.zeros_like(acc_ref)
    rows = acc_ref.shape[2]
    for k in range(slots):
        left = left_ref[pl.ds(k * height, height), :]
        if by_rows:
            pltpu.make_async_copy(part_refs[0].at[0], tile_ref.at[k], sems.at[k, 0]).wait()
        else:
            for n in range(slots):
                pltpu.make_async_copy(part_refs[0].at[0, 0], tile_ref.at[k, n], sems.at[k, n]).wait()
        products = [
            lax.dot_general(
                left,
                tile_ref[k, n],
                (((1,), (0 if by_rows else 1,)), ((), ())),
                preferred_element_type=jnp.float32,
            )
            for n in range(slots)
        ]
        for n in range(slots):
            for q in range(blocks):
                acc_ref[q, targets[k][n]] += products[n][q * rows : (q + 1) * rows]
    me = a if by_rows else b
    for k in range(blocks):
        send_refs[k][...] = acc_ref[me ^ k].astype(jnp.bfloat16)


def product_one(by_rows, index, lefts, parts, blocks, height):
    slab, slots = index.shape
    tile = parts[0].shape[2]
    rows = height // blocks
    message = jax.ShapeDtypeStruct((slab, rows, tile), jnp.bfloat16)
    return pl.pallas_call(
        functools.partial(product_one_kernel, by_rows, len(parts), len(lefts)),
        out_shape=[message] * blocks,
        in_specs=[pl.BlockSpec(memory_space=SMEM)]
        + [pl.BlockSpec(memory_space=VMEM)] * len(lefts)
        + [pl.BlockSpec(memory_space=pl.ANY)] * len(parts),
        out_specs=[pl.BlockSpec(memory_space=VMEM)] * blocks,
        scratch_shapes=[
            pltpu.VMEM(lefts[0].shape, jnp.bfloat16),
            pltpu.VMEM((slots, slots, tile, tile), jnp.bfloat16),
            pltpu.VMEM((blocks, slab, rows, tile), jnp.float32),
            pltpu.SemaphoreType.DMA((slots, slots)),
        ],
        cost_estimate=pl.CostEstimate(flops=12_000_000, bytes_accessed=4_000_000, transcendentals=0),
        name="one_rows" if by_rows else "one_columns",
    )(index, *lefts, *parts)


def product_two_kernel(by_rows, parts, blocks, chunk, index_ref, *refs):
    round_refs, refs = refs[:blocks], refs[blocks:]
    part_refs, refs = refs[:parts], refs[parts:]
    send_refs, (tile_ref, left_ref, sems) = refs[:blocks], refs[blocks:]
    g, a, b = lax.axis_index("gx"), lax.axis_index("gy"), lax.axis_index("gz")
    here = part_refs[0].shape[0]
    slab = here * parts
    slots = tile_ref.shape[1]
    rows = left_ref.shape[2]
    copies = []
    for c in range(slab // chunk):
        t, first = c * chunk // here, c * chunk % here
        copies.append(
            pltpu.make_async_copy(
                part_refs[t].at[pl.ds(first, chunk)], tile_ref.at[pl.ds(c * chunk, chunk)], sems.at[c]
            )
        )
        copies[c].start()
    for k in range(blocks):
        left_ref[a ^ b ^ k] = round_refs[k][...]
    extra = jnp.where(a == b, 3.0, 0.0).astype(jnp.float32)

    def left_of(p):
        return jnp.concatenate([left_ref[m, p] for m in range(blocks)], axis=0)

    def one(q):
        if by_rows:
            entries = [(index_ref[q, j], q, j) for j in range(slots)]
            same = lax.rem(q + here * g, slab)
        else:
            flat = [index_ref[q, n] for n in range(slots)]
            entries = [(e >> 3, e >> 3, e & 7) for e in flat]
            same = lax.rem(q + slab - here * g, slab)
        total = None
        for n in range(0, slots, 2):
            pair = entries[n : n + 2]
            left = jnp.concatenate([left_of(e[0]) for e in pair], axis=1)
            tiles = jnp.concatenate([tile_ref[e[1], e[2]] for e in pair], axis=1 if by_rows else 0)
            product = lax.dot_general(
                left,
                tiles,
                (((1,), (1 if by_rows else 0,)), ((), ())),
                preferred_element_type=jnp.float32,
            )
            total = product if total is None else total + product
        for m in range(blocks):
            value = extra * left_ref[m, same].astype(jnp.float32) - 2.0 * total[m * rows : (m + 1) * rows]
            send_refs[m][q] = value.astype(jnp.bfloat16)

    unroll = 4
    if by_rows:
        for c in range(slab // chunk):
            copies[c].wait()

            @pl.loop(c * chunk, (c + 1) * chunk, step=min(unroll, chunk))
            def _(q):
                for u in range(min(unroll, chunk)):
                    one(q + u)
    else:
        for c in range(slab // chunk):
            copies[c].wait()

        @pl.loop(0, slab, step=unroll)
        def _(q):
            for u in range(unroll):
                one(q + u)


def product_two(by_rows, index, rounded, parts):
    slab, slots = index.shape
    blocks = len(rounded)
    tile = parts[0].shape[2]
    rows = rounded[0].shape[1]
    chunk = min(8, parts[0].shape[0])
    message = jax.ShapeDtypeStruct((slab, rows, tile), jnp.bfloat16)
    return pl.pallas_call(
        functools.partial(product_two_kernel, by_rows, len(parts), blocks, chunk),
        out_shape=[message] * blocks,
        in_specs=[pl.BlockSpec(memory_space=SMEM)]
        + [pl.BlockSpec(memory_space=VMEM)] * blocks
        + [pl.BlockSpec(memory_space=pl.ANY)] * len(parts),
        out_specs=[pl.BlockSpec(memory_space=VMEM)] * blocks,
        scratch_shapes=[
            pltpu.VMEM((slab, slots, tile, tile), jnp.bfloat16),
            pltpu.VMEM((blocks, slab, rows, tile), jnp.bfloat16),
            pltpu.SemaphoreType.DMA((slab // chunk,)),
        ],
        cost_estimate=pl.CostEstimate(flops=30_000_000, bytes_accessed=12_000_000, transcendentals=0),
        name="two_rows" if by_rows else "two_columns",
    )(index, *rounded, *parts)


def finish_kernel(parts, here, *refs):
    half = len(refs) // 2
    first, second, out_ref = refs[:half], refs[half:-1], refs[-1]
    g = lax.axis_index("gx")
    slab, rows, tile = first[0].shape

    def add(refs_in, y):
        total = refs_in[0][y].astype(jnp.float32)
        for ref in refs_in[1:]:
            total = total + ref[y].astype(jnp.float32)
        return total

    @pl.loop(0, slab, unroll=8)
    def _(y):
        columns = pl.ds(pl.multiple_of(y * tile, tile), tile)
        out_ref[0:rows, columns] = add(first, y)
        out_ref[rows : 2 * rows, columns] = add(second, lax.rem(y + slab - here * g, slab))


def finish(first, second, parts, here):
    slab, rows, tile = first[0].shape
    return pl.pallas_call(
        functools.partial(finish_kernel, parts, here),
        out_shape=jax.ShapeDtypeStruct((2 * rows, slab * tile), jnp.float32),
        in_specs=[pl.BlockSpec(memory_space=VMEM)] * (len(first) + len(second)),
        out_specs=pl.BlockSpec(memory_space=VMEM),
        name="finish",
    )(*first, *second)


def total(values):
    summed = values[0].astype(jnp.float32)
    for value in values[1:]:
        summed = summed + value.astype(jnp.float32)
    return summed.astype(jnp.bfloat16)


def local(block_values, block_cols):
    tiles_here = block_values[0, :, 0]
    columns_here = block_cols[0, :, 0]
    here, slots, tile, _ = tiles_here.shape
    parts = lax.axis_size("gx")
    size = lax.axis_size("gy")
    blocks = WIN * tile // size
    rows = blocks // 2
    height = rows * size

    def payload(first):
        window = tiles_here[0].reshape(slots, size, blocks, tile)[:, :, first : first + rows]
        tail = jnp.broadcast_to(columns_here[0].astype(jnp.bfloat16)[:, None], (slots, tile))
        tail = jnp.pad(tail, ((0, 16 - slots), (0, 0)))
        return jnp.concatenate([window.reshape(slots * height, tile), tail], axis=0)

    pay_a, pay_b = payload(0), payload(rows)
    column_parts, tile_parts = [columns_here], [tiles_here]
    for t in range(1, parts):
        shift = [((i + t) % parts, i) for i in range(parts)]
        column_parts.append(lax.ppermute(columns_here, "gx", shift))
    left_a = [pay_a] + [lax.ppermute(pay_a, "gy", [(0, k)]) for k in range(1, size)]
    both = ("gy", "gz")
    left_b = [
        lax.ppermute(pay_b, both, [(a, a * size + (a ^ k)) for a in range(size)]) for k in range(size)
    ]
    for t in range(1, parts):
        shift = [((i + t) % parts, i) for i in range(parts)]
        tile_parts.append(lax.ppermute(tiles_here, "gx", shift))
    columns = jnp.concatenate(column_parts, axis=0)
    inverse = invert(columns)

    def gathered(sends, axis):
        received = [sends[0]] + [
            lax.ppermute(sends[k], axis, swaps(size, k)) for k in range(1, size)
        ]
        own = total(received)
        return [own] + [lax.ppermute(own, axis, swaps(size, k)) for k in range(1, size)]

    sends_a = product_one(False, inverse, left_a, tile_parts, size, height)
    sends_b = product_one(True, columns, left_b, tile_parts, size, height)
    rounded_a = gathered(sends_a, "gz")
    rounded_b = gathered(sends_b, "gy")
    out_b = product_two(True, columns, rounded_b, tile_parts)
    out_a = product_two(False, inverse, rounded_a, tile_parts)
    got_b = [
        lax.ppermute(
            out_b[m],
            both,
            [(a * size + b, (b ^ m) * size + a) for a in range(size) for b in range(size)],
        )
        for m in range(size)
    ]
    got_a = [out_a[0]] + [lax.ppermute(out_a[m], "gy", swaps(size, m)) for m in range(1, size)]
    return finish(got_a, got_b, parts, here)


def solution(mesh):
    in_specs = (P("gy", "gx", "gz", None, None, None), P("gy", "gx", "gz", None))
    out_specs = P(("gx", "gy"), "gz")
    return jax.shard_map(local, mesh=mesh, in_specs=in_specs, out_specs=out_specs, check_vma=False)
```

```python
import functools

import jax
import jax.numpy as jnp
from jax import lax
from jax.experimental import pallas as pl
from jax.experimental.pallas import tpu as pltpu
from jax.sharding import PartitionSpec as P

WIN = 1
UNROLL = 4
VMEM = pltpu.MemorySpace.VMEM
SMEM = pltpu.MemorySpace.SMEM


def limit(mib):
    return pltpu.CompilerParams(vmem_limit_bytes=mib << 20)


def assemble_kernel(parts, *refs):
    part_refs, out_ref, sems = refs[:parts], refs[parts], refs[parts + 1]
    here = part_refs[0].shape[0]
    copies = [
        pltpu.make_async_copy(part_refs[t], out_ref.at[pl.ds(t * here, here)], sems.at[t])
        for t in range(parts)
    ]
    for copy in copies:
        copy.start()
    for copy in copies:
        copy.wait()


def assemble(parts):
    here = parts[0].shape[0]
    shape = (here * len(parts),) + parts[0].shape[1:]
    return pl.pallas_call(
        functools.partial(assemble_kernel, len(parts)),
        out_shape=pltpu.VMEM(shape, jnp.bfloat16),
        in_specs=[pl.BlockSpec(memory_space=pltpu.HBM)] * len(parts),
        out_specs=pl.BlockSpec(memory_space=VMEM),
        scratch_shapes=[pltpu.SemaphoreType.DMA((len(parts),))],
        compiler_params=limit(50),
        cost_estimate=pl.CostEstimate(flops=4_000_000, bytes_accessed=25_000_000, transcendentals=0),
        name="assemble",
    )(*parts)


def swaps(size, step):
    return [(i, i ^ step) for i in range(size)]


def invert_kernel(cols_ref, inv_ref, count_ref):
    rows, slots = cols_ref.shape

    @pl.loop(0, rows)
    def _(y):
        count_ref[y] = 0

    @pl.loop(0, rows)
    def _(p):
        ys = [cols_ref[p, j] for j in range(slots)]
        ns = [count_ref[y] for y in ys]
        for j in range(slots):
            inv_ref[ys[j], ns[j]] = p * 8 + j
        for j in range(slots):
            count_ref[ys[j]] = ns[j] + 1


def invert(columns):
    return pl.pallas_call(
        invert_kernel,
        out_shape=jax.ShapeDtypeStruct(columns.shape, jnp.int32),
        in_specs=[pl.BlockSpec(memory_space=SMEM)],
        out_specs=pl.BlockSpec(memory_space=SMEM),
        scratch_shapes=[pltpu.SMEM((columns.shape[0],), jnp.int32)],
        compiler_params=limit(1),
        cost_estimate=pl.CostEstimate(flops=4_000_000, bytes_accessed=4096, transcendentals=0),
        name="invert",
    )(columns)


def product_one_kernel(by_rows, here, lefts, index_ref, slab_ref, *refs):
    left_refs, refs = refs[:lefts], refs[lefts:]
    blocks = len(refs) - 2
    send_refs, (left_ref, acc_ref) = refs[:blocks], refs[blocks:]
    g, a, b = lax.axis_index("gx"), lax.axis_index("gy"), lax.axis_index("gz")
    slab, slots = slab_ref.shape[:2]
    rows = acc_ref.shape[2]
    height = blocks * rows
    chosen = a ^ b if by_rows else a
    for k in range(lefts):

        @pl.when(chosen == k)
        def _(k=k):
            left_ref[...] = left_refs[k][...]

    tail = left_ref[pl.ds(slots * height, 16), :].astype(jnp.float32)
    columns = [jnp.max(tail[k : k + 1, :]).astype(jnp.int32) for k in range(slots)]
    acc_ref[...] = jnp.zeros_like(acc_ref)
    for k in range(slots):
        left = left_ref[pl.ds(k * height, height), :]
        if by_rows:
            p = lax.rem(columns[k] + slab - here * g, slab)
            targets = [index_ref[p, j] for j in range(slots)]
            tiles = [slab_ref[p, j] for j in range(slots)]
        else:
            entries = [index_ref[columns[k], n] for n in range(slots)]
            targets = [entry >> 3 for entry in entries]
            tiles = [slab_ref[entry >> 3, entry & 7] for entry in entries]
        products = [
            lax.dot_general(
                left,
                tile,
                (((1,), (0 if by_rows else 1,)), ((), ())),
                preferred_element_type=jnp.float32,
            )
            for tile in tiles
        ]
        for n in range(slots):
            for q in range(blocks):
                acc_ref[q, targets[n]] += products[n][q * rows : (q + 1) * rows]
    me = a if by_rows else b
    for k in range(blocks):
        send_refs[k][...] = acc_ref[me ^ k].astype(jnp.bfloat16)


def product_one(by_rows, index, lefts, tiles, here, blocks, height):
    slab, _ = index.shape
    tile = tiles.shape[2]
    rows = height // blocks
    message = jax.ShapeDtypeStruct((slab, rows, tile), jnp.bfloat16)
    return pl.pallas_call(
        functools.partial(product_one_kernel, by_rows, here, len(lefts)),
        out_shape=[message] * blocks,
        in_specs=[pl.BlockSpec(memory_space=SMEM)]
        + [pl.BlockSpec(memory_space=VMEM)] * (1 + len(lefts)),
        out_specs=[pl.BlockSpec(memory_space=VMEM)] * blocks,
        scratch_shapes=[
            pltpu.VMEM(lefts[0].shape, jnp.bfloat16),
            pltpu.VMEM((blocks, slab, rows, tile), jnp.float32),
        ],
        compiler_params=limit(20),
        cost_estimate=pl.CostEstimate(flops=12_000_000, bytes_accessed=4_000_000, transcendentals=0),
        name="one_rows" if by_rows else "one_columns",
    )(index, tiles, *lefts)


def product_two_kernel(by_rows, here, blocks, index_ref, slab_ref, *refs):
    round_refs, refs = refs[:blocks], refs[blocks:]
    send_refs, (left_ref,) = refs[:blocks], refs[blocks:]
    g, a, b = lax.axis_index("gx"), lax.axis_index("gy"), lax.axis_index("gz")
    slab, slots = slab_ref.shape[:2]
    rows = left_ref.shape[2]
    for k in range(blocks):
        left_ref[a ^ b ^ k] = round_refs[k][...]
    extra = jnp.where(a == b, 3.0, 0.0).astype(jnp.float32)

    def left_of(p):
        return jnp.concatenate([left_ref[m, p] for m in range(blocks)], axis=0)

    def one(q, lefts, tiles, same):
        summed = None
        for n in range(0, slots, 2):
            left = jnp.concatenate([left_of(p) for p in lefts[n : n + 2]], axis=1)
            pair = jnp.concatenate(tiles[n : n + 2], axis=1 if by_rows else 0)
            product = lax.dot_general(
                left,
                pair,
                (((1,), (1 if by_rows else 0,)), ((), ())),
                preferred_element_type=jnp.float32,
            )
            summed = product if summed is None else summed + product
        for m in range(blocks):
            value = extra * left_ref[m, same].astype(jnp.float32) - 2.0 * summed[m * rows : (m + 1) * rows]
            send_refs[m][q] = value.astype(jnp.bfloat16)

    @pl.loop(0, slab, step=UNROLL)
    def _(first):
        for u in range(UNROLL):
            q = first + u
            entries = [index_ref[q, n] for n in range(slots)]
            if by_rows:
                tiles = [slab_ref[q, j] for j in range(slots)]
                one(q, entries, tiles, lax.rem(q + here * g, slab))
            else:
                lefts = [entry >> 3 for entry in entries]
                tiles = [slab_ref[entry >> 3, entry & 7] for entry in entries]
                one(q, lefts, tiles, lax.rem(q + slab - here * g, slab))


def product_two(by_rows, index, rounded, tiles, here):
    slab, _ = index.shape
    blocks = len(rounded)
    tile = tiles.shape[2]
    rows = rounded[0].shape[1]
    message = jax.ShapeDtypeStruct((slab, rows, tile), jnp.bfloat16)
    return pl.pallas_call(
        functools.partial(product_two_kernel, by_rows, here, blocks),
        out_shape=[message] * blocks,
        in_specs=[pl.BlockSpec(memory_space=SMEM)]
        + [pl.BlockSpec(memory_space=VMEM)] * (1 + blocks),
        out_specs=[pl.BlockSpec(memory_space=VMEM)] * blocks,
        scratch_shapes=[pltpu.VMEM((blocks, slab, rows, tile), jnp.bfloat16)],
        compiler_params=limit(20),
        cost_estimate=pl.CostEstimate(flops=30_000_000, bytes_accessed=12_000_000, transcendentals=0),
        name="two_rows" if by_rows else "two_columns",
    )(index, tiles, *rounded)


def finish_kernel(here, *refs):
    half = len(refs) // 2
    first, second, out_ref = refs[:half], refs[half:-1], refs[-1]
    g = lax.axis_index("gx")
    slab, rows, tile = first[0].shape

    def add(refs_in, y):
        total = refs_in[0][y].astype(jnp.float32)
        for ref in refs_in[1:]:
            total = total + ref[y].astype(jnp.float32)
        return total

    @pl.loop(0, slab, unroll=8)
    def _(y):
        columns = pl.ds(pl.multiple_of(y * tile, tile), tile)
        out_ref[0:rows, columns] = add(first, y)
        out_ref[rows : 2 * rows, columns] = add(second, lax.rem(y + slab - here * g, slab))


def finish(first, second, here):
    slab, rows, tile = first[0].shape
    return pl.pallas_call(
        functools.partial(finish_kernel, here),
        out_shape=jax.ShapeDtypeStruct((2 * rows, slab * tile), jnp.float32),
        in_specs=[pl.BlockSpec(memory_space=VMEM)] * (len(first) + len(second)),
        out_specs=pl.BlockSpec(memory_space=VMEM),
        compiler_params=limit(8),
        name="finish",
    )(*first, *second)


def total(values):
    summed = values[0].astype(jnp.float32)
    for value in values[1:]:
        summed = summed + value.astype(jnp.float32)
    return summed.astype(jnp.bfloat16)


def local(block_values, block_cols):
    tiles_here = block_values[0, :, 0]
    columns_here = block_cols[0, :, 0]
    here, slots, tile, _ = tiles_here.shape
    parts = lax.axis_size("gx")
    size = lax.axis_size("gy")
    blocks = WIN * tile // size
    rows = blocks // 2
    height = rows * size

    def payload(first):
        window = tiles_here[0].reshape(slots, size, blocks, tile)[:, :, first : first + rows]
        tail = jnp.broadcast_to(columns_here[0].astype(jnp.bfloat16)[:, None], (slots, tile))
        tail = jnp.pad(tail, ((0, 16 - slots), (0, 0)))
        return jnp.concatenate([window.reshape(slots * height, tile), tail], axis=0)

    pay_a, pay_b = payload(0), payload(rows)
    both = ("gy", "gz")
    shifts = [[((i + t) % parts, i) for i in range(parts)] for t in range(1, parts)]
    left_a = [pay_a] + [lax.ppermute(pay_a, "gy", [(0, k)]) for k in range(1, size)]
    columns = jnp.concatenate([columns_here] + [lax.ppermute(columns_here, "gx", s) for s in shifts], axis=0)
    inverse = invert(columns)
    moved = [lax.ppermute(tiles_here, "gx", s) for s in shifts]
    left_b = [
        lax.ppermute(pay_b, both, [(a, a * size + (a ^ k)) for a in range(size)]) for k in range(size)
    ]
    tiles = assemble([tiles_here] + moved)

    def scatter(sends, axis):
        return [sends[0]] + [lax.ppermute(sends[k], axis, swaps(size, k)) for k in range(1, size)]

    def spread(own, axis):
        return [own] + [lax.ppermute(own, axis, swaps(size, k)) for k in range(1, size)]

    sends_a = product_one(False, inverse, left_a, tiles, here, size, height)
    parts_a = scatter(sends_a, "gz")
    _, left_b = lax.optimization_barrier((sends_a[0], left_b))
    sends_b = product_one(True, columns, left_b, tiles, here, size, height)
    parts_b = scatter(sends_b, "gy")
    own_b = total(parts_b)
    own_a = total(parts_a)
    rounded_b = spread(own_b, "gy")
    rounded_a = spread(own_a, "gz")
    out_b = product_two(True, columns, rounded_b, tiles, here)
    got_b = [
        lax.ppermute(
            out_b[m],
            both,
            [(a * size + b, (b ^ m) * size + a) for a in range(size) for b in range(size)],
        )
        for m in range(size)
    ]
    out_a = product_two(False, inverse, rounded_a, tiles, here)
    got_a = scatter(out_a, "gy")
    return finish(got_a, got_b, here)


def solution(mesh):
    in_specs = (P("gy", "gx", "gz", None, None, None), P("gy", "gx", "gz", None))
    out_specs = P(("gx", "gy"), "gz")
    return jax.shard_map(local, mesh=mesh, in_specs=in_specs, out_specs=out_specs, check_vma=False)
```

```python
import functools

import jax
import jax.numpy as jnp
from jax import lax
from jax.experimental import pallas as pl
from jax.experimental.pallas import tpu as pltpu
from jax.sharding import PartitionSpec as P

WIN = 1
UNROLL = 4
VMEM = pltpu.MemorySpace.VMEM
SMEM = pltpu.MemorySpace.SMEM


def limit(mib):
    return pltpu.CompilerParams(vmem_limit_bytes=mib << 20)


def assemble_kernel(parts, *refs):
    part_refs, out_ref, sems = refs[:parts], refs[parts], refs[parts + 1]
    here = part_refs[0].shape[0]
    copies = [
        pltpu.make_async_copy(part_refs[t], out_ref.at[pl.ds(t * here, here)], sems.at[t])
        for t in range(parts)
    ]
    for copy in copies:
        copy.start()
    for copy in copies:
        copy.wait()


def assemble(parts):
    here = parts[0].shape[0]
    shape = (here * len(parts),) + parts[0].shape[1:]
    return pl.pallas_call(
        functools.partial(assemble_kernel, len(parts)),
        out_shape=pltpu.VMEM(shape, jnp.bfloat16),
        in_specs=[pl.BlockSpec(memory_space=pltpu.HBM)] * len(parts),
        out_specs=pl.BlockSpec(memory_space=VMEM),
        scratch_shapes=[pltpu.SemaphoreType.DMA((len(parts),))],
        compiler_params=limit(50),
        cost_estimate=pl.CostEstimate(flops=4_000_000, bytes_accessed=25_000_000, transcendentals=0),
        name="assemble",
    )(*parts)


def pick_kernel(*refs):
    blocks = len(refs) // 2
    a, b = lax.axis_index("gy"), lax.axis_index("gz")
    for m in range(blocks):
        for k in range(blocks):

            @pl.when(a ^ b ^ k == m)
            def _(k=k, m=m):
                refs[blocks + k][...] = refs[m][...]


def pick(values):
    return pl.pallas_call(
        pick_kernel,
        out_shape=[jax.ShapeDtypeStruct(value.shape, value.dtype) for value in values],
        in_specs=[pl.BlockSpec(memory_space=VMEM)] * len(values),
        out_specs=[pl.BlockSpec(memory_space=VMEM)] * len(values),
        compiler_params=limit(8),
        cost_estimate=pl.CostEstimate(flops=1_000_000, bytes_accessed=2_000_000, transcendentals=0),
        name="pick",
    )(*values)


def swaps(size, step):
    return [(i, i ^ step) for i in range(size)]


def invert_kernel(cols_ref, inv_ref, count_ref):
    rows, slots = cols_ref.shape

    @pl.loop(0, rows)
    def _(y):
        count_ref[y] = 0

    @pl.loop(0, rows)
    def _(p):
        ys = [cols_ref[p, j] for j in range(slots)]
        ns = [count_ref[y] for y in ys]
        for j in range(slots):
            inv_ref[ys[j], ns[j]] = p * 8 + j
        for j in range(slots):
            count_ref[ys[j]] = ns[j] + 1


def invert(columns):
    return pl.pallas_call(
        invert_kernel,
        out_shape=jax.ShapeDtypeStruct(columns.shape, jnp.int32),
        in_specs=[pl.BlockSpec(memory_space=SMEM)],
        out_specs=pl.BlockSpec(memory_space=SMEM),
        scratch_shapes=[pltpu.SMEM((columns.shape[0],), jnp.int32)],
        compiler_params=limit(1),
        cost_estimate=pl.CostEstimate(flops=4_000_000, bytes_accessed=4096, transcendentals=0),
        name="invert",
    )(columns)


def product_one_kernel(by_rows, here, lefts, index_ref, slab_ref, *refs):
    left_refs, refs = refs[:lefts], refs[lefts:]
    blocks = len(refs) - 2
    send_refs, (left_ref, acc_ref) = refs[:blocks], refs[blocks:]
    g, a, b = lax.axis_index("gx"), lax.axis_index("gy"), lax.axis_index("gz")
    slab, slots = slab_ref.shape[:2]
    rows = acc_ref.shape[2]
    height = blocks * rows
    chosen = a ^ b if by_rows else a
    for k in range(lefts):

        @pl.when(chosen == k)
        def _(k=k):
            left_ref[...] = left_refs[k][...]

    tail = left_ref[pl.ds(slots * height, 16), :].astype(jnp.float32)
    columns = [jnp.max(tail[k : k + 1, :]).astype(jnp.int32) for k in range(slots)]
    acc_ref[...] = jnp.zeros_like(acc_ref)
    for k in range(slots):
        left = left_ref[pl.ds(k * height, height), :]
        if by_rows:
            p = lax.rem(columns[k] + slab - here * g, slab)
            targets = [index_ref[p, j] for j in range(slots)]
            tiles = [slab_ref[p, j] for j in range(slots)]
        else:
            entries = [index_ref[columns[k], n] for n in range(slots)]
            targets = [entry >> 3 for entry in entries]
            tiles = [slab_ref[entry >> 3, entry & 7] for entry in entries]
        products = [
            lax.dot_general(
                left,
                tile,
                (((1,), (0 if by_rows else 1,)), ((), ())),
                preferred_element_type=jnp.float32,
            )
            for tile in tiles
        ]
        for n in range(slots):
            for q in range(blocks):
                acc_ref[q, targets[n]] += products[n][q * rows : (q + 1) * rows]
    me = a if by_rows else b
    for k in range(blocks):
        send_refs[k][...] = acc_ref[me ^ k].astype(jnp.bfloat16)


def product_one(by_rows, index, lefts, tiles, here, blocks, height):
    slab, _ = index.shape
    tile = tiles.shape[2]
    rows = height // blocks
    message = jax.ShapeDtypeStruct((slab, rows, tile), jnp.bfloat16)
    return pl.pallas_call(
        functools.partial(product_one_kernel, by_rows, here, len(lefts)),
        out_shape=[message] * blocks,
        in_specs=[pl.BlockSpec(memory_space=SMEM)]
        + [pl.BlockSpec(memory_space=VMEM)] * (1 + len(lefts)),
        out_specs=[pl.BlockSpec(memory_space=VMEM)] * blocks,
        scratch_shapes=[
            pltpu.VMEM(lefts[0].shape, jnp.bfloat16),
            pltpu.VMEM((blocks, slab, rows, tile), jnp.float32),
        ],
        compiler_params=limit(20),
        cost_estimate=pl.CostEstimate(flops=12_000_000, bytes_accessed=4_000_000, transcendentals=0),
        name="one_rows" if by_rows else "one_columns",
    )(index, tiles, *lefts)


def product_two_kernel(by_rows, here, blocks, index_ref, slab_ref, *refs):
    round_refs, refs = refs[:blocks], refs[blocks:]
    send_refs, (left_ref,) = refs[:blocks], refs[blocks:]
    g, a, b = lax.axis_index("gx"), lax.axis_index("gy"), lax.axis_index("gz")
    slab, slots = slab_ref.shape[:2]
    rows = left_ref.shape[2]
    for k in range(blocks):
        left_ref[k if by_rows else a ^ b ^ k] = round_refs[k][...]
    extra = jnp.where(a == b, 3.0, 0.0).astype(jnp.float32)

    def left_of(p):
        return jnp.concatenate([left_ref[m, p] for m in range(blocks)], axis=0)

    def one(q, lefts, tiles, same):
        summed = None
        for n in range(0, slots, 2):
            left = jnp.concatenate([left_of(p) for p in lefts[n : n + 2]], axis=1)
            pair = jnp.concatenate(tiles[n : n + 2], axis=1 if by_rows else 0)
            product = lax.dot_general(
                left,
                pair,
                (((1,), (1 if by_rows else 0,)), ((), ())),
                preferred_element_type=jnp.float32,
            )
            summed = product if summed is None else summed + product
        for m in range(blocks):
            value = extra * left_ref[m, same].astype(jnp.float32) - 2.0 * summed[m * rows : (m + 1) * rows]
            send_refs[m][q] = value.astype(jnp.bfloat16)

    @pl.loop(0, slab, step=UNROLL)
    def _(first):
        for u in range(UNROLL):
            q = first + u
            entries = [index_ref[q, n] for n in range(slots)]
            if by_rows:
                tiles = [slab_ref[q, j] for j in range(slots)]
                one(q, entries, tiles, lax.rem(q + here * g, slab))
            else:
                lefts = [entry >> 3 for entry in entries]
                tiles = [slab_ref[entry >> 3, entry & 7] for entry in entries]
                one(q, lefts, tiles, lax.rem(q + slab - here * g, slab))


def product_two(by_rows, index, rounded, tiles, here):
    slab, _ = index.shape
    blocks = len(rounded)
    tile = tiles.shape[2]
    rows = rounded[0].shape[1]
    message = jax.ShapeDtypeStruct((slab, rows, tile), jnp.bfloat16)
    return pl.pallas_call(
        functools.partial(product_two_kernel, by_rows, here, blocks),
        out_shape=[message] * blocks,
        in_specs=[pl.BlockSpec(memory_space=SMEM)]
        + [pl.BlockSpec(memory_space=VMEM)] * (1 + blocks),
        out_specs=[pl.BlockSpec(memory_space=VMEM)] * blocks,
        scratch_shapes=[pltpu.VMEM((blocks, slab, rows, tile), jnp.bfloat16)],
        compiler_params=limit(20),
        cost_estimate=pl.CostEstimate(flops=30_000_000, bytes_accessed=12_000_000, transcendentals=0),
        name="two_rows" if by_rows else "two_columns",
    )(index, tiles, *rounded)


def finish_kernel(here, *refs):
    half = len(refs) // 2
    first, second, out_ref = refs[:half], refs[half:-1], refs[-1]
    g = lax.axis_index("gx")
    slab, rows, tile = first[0].shape

    def add(refs_in, y):
        total = refs_in[0][y].astype(jnp.float32)
        for ref in refs_in[1:]:
            total = total + ref[y].astype(jnp.float32)
        return total

    @pl.loop(0, slab, unroll=8)
    def _(y):
        columns = pl.ds(pl.multiple_of(y * tile, tile), tile)
        out_ref[0:rows, columns] = add(first, y)
        out_ref[rows : 2 * rows, columns] = add(second, lax.rem(y + slab - here * g, slab))


def finish(first, second, here):
    slab, rows, tile = first[0].shape
    return pl.pallas_call(
        functools.partial(finish_kernel, here),
        out_shape=jax.ShapeDtypeStruct((2 * rows, slab * tile), jnp.float32),
        in_specs=[pl.BlockSpec(memory_space=VMEM)] * (len(first) + len(second)),
        out_specs=pl.BlockSpec(memory_space=VMEM),
        compiler_params=limit(8),
        name="finish",
    )(*first, *second)


def total(values):
    summed = values[0].astype(jnp.float32)
    for value in values[1:]:
        summed = summed + value.astype(jnp.float32)
    return summed.astype(jnp.bfloat16)


def local(block_values, block_cols):
    tiles_here = block_values[0, :, 0]
    columns_here = block_cols[0, :, 0]
    here, slots, tile, _ = tiles_here.shape
    parts = lax.axis_size("gx")
    size = lax.axis_size("gy")
    blocks = WIN * tile // size
    rows = blocks // 2
    height = rows * size

    def payload(first):
        window = tiles_here[0].reshape(slots, size, blocks, tile)[:, :, first : first + rows]
        tail = jnp.broadcast_to(columns_here[0].astype(jnp.bfloat16)[:, None], (slots, tile))
        tail = jnp.pad(tail, ((0, 16 - slots), (0, 0)))
        return jnp.concatenate([window.reshape(slots * height, tile), tail], axis=0)

    pay_a, pay_b = payload(0), payload(rows)
    both = ("gy", "gz")
    shifts = [[((i + t) % parts, i) for i in range(parts)] for t in range(1, parts)]
    others = [lax.ppermute(columns_here, "gx", s) for s in shifts]
    moved = [lax.ppermute(tiles_here, "gx", s) for s in shifts]
    left_a = [pay_a] + [lax.ppermute(pay_a, "gy", [(0, k)]) for k in range(1, size)]
    left_b = [
        lax.ppermute(pay_b, both, [(a, a * size + (a ^ k)) for a in range(size)]) for k in range(size)
    ]
    columns = jnp.concatenate([columns_here] + others, axis=0)
    inverse = invert(columns)
    tiles = assemble([tiles_here] + moved)

    def scatter(sends, axis):
        return [sends[0]] + [lax.ppermute(sends[k], axis, swaps(size, k)) for k in range(1, size)]

    def spread(own, axis):
        return [own] + [lax.ppermute(own, axis, swaps(size, k)) for k in range(1, size)]

    sends_a = product_one(False, inverse, left_a, tiles, here, size, height)
    parts_a = scatter(sends_a, "gz")
    _, left_b = lax.optimization_barrier((sends_a[0], left_b))
    sends_b = product_one(True, columns, left_b, tiles, here, size, height)
    parts_b = scatter(sends_b, "gy")
    own_b = total(parts_b)
    own_a = total(parts_a)
    rounded_b = spread(own_b, "gy")
    rounded_a = spread(own_a, "gz")
    out_b = product_two(True, columns, rounded_b, tiles, here)
    crossed = scatter(out_b, "gy")
    picked = pick(crossed)
    got_b = scatter(picked, "gz")
    out_a = product_two(False, inverse, rounded_a, tiles, here)
    got_a = scatter(out_a, "gy")
    return finish(got_a, got_b, here)


def solution(mesh):
    in_specs = (P("gy", "gx", "gz", None, None, None), P("gy", "gx", "gz", None))
    out_specs = P(("gx", "gy"), "gz")
    return jax.shard_map(local, mesh=mesh, in_specs=in_specs, out_specs=out_specs, check_vma=False)
```

```python
import functools

import jax
import jax.numpy as jnp
from jax import lax
from jax.experimental import pallas as pl
from jax.experimental.pallas import tpu as pltpu
from jax.sharding import PartitionSpec as P

WIN = 1
UNROLL = 4
VMEM = pltpu.MemorySpace.VMEM
SMEM = pltpu.MemorySpace.SMEM


def limit(mib):
    return pltpu.CompilerParams(vmem_limit_bytes=mib << 20)


def assemble_kernel(parts, *refs):
    part_refs, out_ref, sems = refs[:parts], refs[parts], refs[parts + 1]
    here = part_refs[0].shape[0]
    copies = [
        pltpu.make_async_copy(part_refs[t], out_ref.at[pl.ds(t * here, here)], sems.at[t])
        for t in range(parts)
    ]
    for copy in copies:
        copy.start()
    for copy in copies:
        copy.wait()


def assemble(parts):
    here = parts[0].shape[0]
    shape = (here * len(parts),) + parts[0].shape[1:]
    return pl.pallas_call(
        functools.partial(assemble_kernel, len(parts)),
        out_shape=pltpu.VMEM(shape, jnp.bfloat16),
        in_specs=[pl.BlockSpec(memory_space=pltpu.HBM)] * len(parts),
        out_specs=pl.BlockSpec(memory_space=VMEM),
        scratch_shapes=[pltpu.SemaphoreType.DMA((len(parts),))],
        compiler_params=limit(46),
        cost_estimate=pl.CostEstimate(flops=4_000_000, bytes_accessed=25_000_000, transcendentals=0),
        name="assemble",
    )(*parts)


def pick_kernel(*refs):
    blocks = len(refs) // 2
    a, b = lax.axis_index("gy"), lax.axis_index("gz")
    for m in range(blocks):
        for k in range(blocks):

            @pl.when(a ^ b ^ k == m)
            def _(k=k, m=m):
                refs[blocks + k][...] = refs[m][...]


def pick(values):
    return pl.pallas_call(
        pick_kernel,
        out_shape=[jax.ShapeDtypeStruct(value.shape, value.dtype) for value in values],
        in_specs=[pl.BlockSpec(memory_space=VMEM)] * len(values),
        out_specs=[pl.BlockSpec(memory_space=VMEM)] * len(values),
        compiler_params=limit(8),
        cost_estimate=pl.CostEstimate(flops=1_000_000, bytes_accessed=2_000_000, transcendentals=0),
        name="pick",
    )(*values)


def swaps(size, step):
    return [(i, i ^ step) for i in range(size)]


def invert_kernel(cols_ref, inv_ref):
    rows, slots = cols_ref.shape
    count = rows * slots
    lane = lax.broadcasted_iota(jnp.int32, (rows, 128), 1)
    hits = jnp.concatenate(
        [(cols_ref[:, j : j + 1] == lane).astype(jnp.float32) for j in range(slots)], axis=0
    )
    above = lax.broadcasted_iota(jnp.int32, (count, count), 0) > lax.broadcasted_iota(
        jnp.int32, (count, count), 1
    )
    rank = jnp.dot(
        above.astype(jnp.bfloat16), hits.astype(jnp.bfloat16), preferred_element_type=jnp.float32
    )
    code = jnp.concatenate(
        [lax.broadcasted_iota(jnp.int32, (rows, 128), 0) * 8 + j for j in range(slots)], axis=0
    ).astype(jnp.float32)
    code = code * hits
    lines = [
        jnp.sum(jnp.where(rank == n, code, 0.0), axis=0, keepdims=True) for n in range(slots)
    ]
    lines += [jnp.zeros_like(lines[0])] * (8 - slots)
    inv_ref[...] = jnp.concatenate(lines, axis=0).astype(jnp.int32)


def invert(columns):
    return pl.pallas_call(
        invert_kernel,
        out_shape=jax.ShapeDtypeStruct((8, 128), jnp.int32),
        in_specs=[pl.BlockSpec(memory_space=VMEM)],
        out_specs=pl.BlockSpec(memory_space=VMEM),
        compiler_params=limit(4),
        cost_estimate=pl.CostEstimate(flops=4_000_000, bytes_accessed=4096, transcendentals=0),
        name="invert",
    )(columns)


def product_one_kernel(by_rows, lefts, parts, index_ref, *refs):
    left_refs, refs = refs[:lefts], refs[lefts:]
    part_refs, refs = refs[:parts], refs[parts:]
    blocks = len(refs) - 4
    send_refs, (left_ref, tile_ref, acc_ref, sems) = refs[:blocks], refs[blocks:]
    g, a, b = lax.axis_index("gx"), lax.axis_index("gy"), lax.axis_index("gz")
    here, slots = part_refs[0].shape[:2]
    slab = here * parts
    rows = acc_ref.shape[2]
    height = blocks * rows
    chosen = a ^ b if by_rows else a
    for k in range(lefts):

        @pl.when(chosen == k)
        def _(k=k):
            left_ref[...] = left_refs[k][...]

    tail = left_ref[pl.ds(slots * height, 16), :].astype(jnp.float32)
    columns = [jnp.max(tail[k : k + 1, :]).astype(jnp.int32) for k in range(slots)]
    targets = []
    for k in range(slots):
        if by_rows:
            p = lax.rem(columns[k] + slab - here * g, slab)
            targets.append([index_ref[p, j] for j in range(slots)])
            for t in range(parts):

                @pl.when(p // here == t)
                def _(k=k, t=t, p=p):
                    pltpu.make_async_copy(
                        part_refs[t].at[lax.rem(p, here)], tile_ref.at[k], sems.at[k, 0]
                    ).start()

        else:
            entries = [index_ref[n, columns[k]] for n in range(slots)]
            targets.append([entry >> 3 for entry in entries])
            for n in range(slots):
                p, j = entries[n] >> 3, entries[n] & 7
                for t in range(parts):

                    @pl.when(p // here == t)
                    def _(k=k, n=n, t=t, p=p, j=j):
                        pltpu.make_async_copy(
                            part_refs[t].at[lax.rem(p, here), j], tile_ref.at[k, n], sems.at[k, n]
                        ).start()

    acc_ref[...] = jnp.zeros_like(acc_ref)
    for k in range(slots):
        left = left_ref[pl.ds(k * height, height), :]
        if by_rows:
            pltpu.make_async_copy(part_refs[0].at[0], tile_ref.at[k], sems.at[k, 0]).wait()
        else:
            for n in range(slots):
                pltpu.make_async_copy(part_refs[0].at[0, 0], tile_ref.at[k, n], sems.at[k, n]).wait()
        products = [
            lax.dot_general(
                left,
                tile_ref[k, n],
                (((1,), (0 if by_rows else 1,)), ((), ())),
                preferred_element_type=jnp.float32,
            )
            for n in range(slots)
        ]
        for n in range(slots):
            for q in range(blocks):
                acc_ref[q, targets[k][n]] += products[n][q * rows : (q + 1) * rows]
    me = a if by_rows else b
    for k in range(blocks):
        send_refs[k][...] = acc_ref[me ^ k].astype(jnp.bfloat16)


def product_one(by_rows, index, lefts, parts, blocks, height):
    here, slots, tile = parts[0].shape[:3]
    slab = here * len(parts)
    rows = height // blocks
    message = jax.ShapeDtypeStruct((slab, rows, tile), jnp.bfloat16)
    return pl.pallas_call(
        functools.partial(product_one_kernel, by_rows, len(lefts), len(parts)),
        out_shape=[message] * blocks,
        in_specs=[pl.BlockSpec(memory_space=SMEM)]
        + [pl.BlockSpec(memory_space=VMEM)] * len(lefts)
        + [pl.BlockSpec(memory_space=pltpu.HBM)] * len(parts),
        out_specs=[pl.BlockSpec(memory_space=VMEM)] * blocks,
        scratch_shapes=[
            pltpu.VMEM(lefts[0].shape, jnp.bfloat16),
            pltpu.VMEM((slots, slots, tile, tile), jnp.bfloat16),
            pltpu.VMEM((blocks, slab, rows, tile), jnp.float32),
            pltpu.SemaphoreType.DMA((slots, slots)),
        ],
        compiler_params=limit(50),
        cost_estimate=pl.CostEstimate(flops=12_000_000, bytes_accessed=4_000_000, transcendentals=0),
        name="one_rows" if by_rows else "one_columns",
    )(index, *lefts, *parts)


def product_two_kernel(by_rows, here, blocks, index_ref, slab_ref, *refs):
    round_refs, refs = refs[:blocks], refs[blocks:]
    send_refs, (left_ref,) = refs[:blocks], refs[blocks:]
    g, a, b = lax.axis_index("gx"), lax.axis_index("gy"), lax.axis_index("gz")
    slab, slots = slab_ref.shape[:2]
    rows = left_ref.shape[2]
    for k in range(blocks):
        left_ref[k if by_rows else a ^ b ^ k] = round_refs[k][...]
    extra = jnp.where(a == b, 3.0, 0.0).astype(jnp.float32)

    def left_of(p):
        return jnp.concatenate([left_ref[m, p] for m in range(blocks)], axis=0)

    def one(q, lefts, tiles, same):
        summed = None
        for n in range(0, slots, 2):
            left = jnp.concatenate([left_of(p) for p in lefts[n : n + 2]], axis=1)
            pair = jnp.concatenate(tiles[n : n + 2], axis=1 if by_rows else 0)
            product = lax.dot_general(
                left,
                pair,
                (((1,), (1 if by_rows else 0,)), ((), ())),
                preferred_element_type=jnp.float32,
            )
            summed = product if summed is None else summed + product
        for m in range(blocks):
            value = extra * left_ref[m, same].astype(jnp.float32) - 2.0 * summed[m * rows : (m + 1) * rows]
            send_refs[m][q] = value.astype(jnp.bfloat16)

    @pl.loop(0, slab, step=UNROLL)
    def _(first):
        for u in range(UNROLL):
            q = first + u
            entries = [index_ref[q, n] if by_rows else index_ref[n, q] for n in range(slots)]
            if by_rows:
                tiles = [slab_ref[q, j] for j in range(slots)]
                one(q, entries, tiles, lax.rem(q + here * g, slab))
            else:
                lefts = [entry >> 3 for entry in entries]
                tiles = [slab_ref[entry >> 3, entry & 7] for entry in entries]
                one(q, lefts, tiles, lax.rem(q + slab - here * g, slab))


def product_two(by_rows, index, rounded, tiles, here):
    slab, _, tile = tiles.shape[:3]
    blocks = len(rounded)
    rows = rounded[0].shape[1]
    message = jax.ShapeDtypeStruct((slab, rows, tile), jnp.bfloat16)
    return pl.pallas_call(
        functools.partial(product_two_kernel, by_rows, here, blocks),
        out_shape=[message] * blocks,
        in_specs=[pl.BlockSpec(memory_space=SMEM)]
        + [pl.BlockSpec(memory_space=VMEM)] * (1 + blocks),
        out_specs=[pl.BlockSpec(memory_space=VMEM)] * blocks,
        scratch_shapes=[pltpu.VMEM((blocks, slab, rows, tile), jnp.bfloat16)],
        compiler_params=limit(20),
        cost_estimate=pl.CostEstimate(flops=30_000_000, bytes_accessed=12_000_000, transcendentals=0),
        name="two_rows" if by_rows else "two_columns",
    )(index, tiles, *rounded)


def finish_kernel(here, *refs):
    half = len(refs) // 2
    first, second, out_ref = refs[:half], refs[half:-1], refs[-1]
    g = lax.axis_index("gx")
    slab, rows, tile = first[0].shape

    def add(refs_in, y):
        total = refs_in[0][y].astype(jnp.float32)
        for ref in refs_in[1:]:
            total = total + ref[y].astype(jnp.float32)
        return total

    @pl.loop(0, slab, unroll=8)
    def _(y):
        columns = pl.ds(pl.multiple_of(y * tile, tile), tile)
        out_ref[0:rows, columns] = add(first, y)
        out_ref[rows : 2 * rows, columns] = add(second, lax.rem(y + slab - here * g, slab))


def finish(first, second, here):
    slab, rows, tile = first[0].shape
    return pl.pallas_call(
        functools.partial(finish_kernel, here),
        out_shape=jax.ShapeDtypeStruct((2 * rows, slab * tile), jnp.float32),
        in_specs=[pl.BlockSpec(memory_space=VMEM)] * (len(first) + len(second)),
        out_specs=pl.BlockSpec(memory_space=VMEM),
        compiler_params=limit(8),
        name="finish",
    )(*first, *second)


def total(values):
    summed = values[0].astype(jnp.float32)
    for value in values[1:]:
        summed = summed + value.astype(jnp.float32)
    return summed.astype(jnp.bfloat16)


def local(block_values, block_cols):
    tiles_here = block_values[0, :, 0]
    columns_here = block_cols[0, :, 0]
    here, slots, tile, _ = tiles_here.shape
    parts = lax.axis_size("gx")
    size = lax.axis_size("gy")
    blocks = WIN * tile // size
    rows = blocks // 2
    height = rows * size

    def payload(first):
        window = tiles_here[0].reshape(slots, size, blocks, tile)[:, :, first : first + rows]
        tail = jnp.broadcast_to(columns_here[0].astype(jnp.bfloat16)[:, None], (slots, tile))
        tail = jnp.pad(tail, ((0, 16 - slots), (0, 0)))
        return jnp.concatenate([window.reshape(slots * height, tile), tail], axis=0)

    pay_a, pay_b = payload(0), payload(rows)
    both = ("gy", "gz")
    shifts = [[((i + t) % parts, i) for i in range(parts)] for t in range(1, parts)]
    others = [lax.ppermute(columns_here, "gx", s) for s in shifts]
    moved = [lax.ppermute(tiles_here, "gx", s) for s in shifts]
    left_b = [
        lax.ppermute(pay_b, both, [(a, a * size + (a ^ k)) for a in range(size)]) for k in range(size)
    ]
    left_a = [pay_a] + [lax.ppermute(pay_a, "gy", [(0, k)]) for k in range(1, size)]
    columns = jnp.concatenate([columns_here] + others, axis=0)
    inverse = invert(columns)
    pieces = [tiles_here] + moved

    def scatter(sends, axis):
        return [sends[0]] + [lax.ppermute(sends[k], axis, swaps(size, k)) for k in range(1, size)]

    def spread(own, axis):
        return [own] + [lax.ppermute(own, axis, swaps(size, k)) for k in range(1, size)]

    sends_b = product_one(True, columns, left_b, pieces, size, height)
    parts_b = scatter(sends_b, "gy")
    _, left_a = lax.optimization_barrier((sends_b[0], left_a))
    sends_a = product_one(False, inverse, left_a, pieces, size, height)
    parts_a = scatter(sends_a, "gz")
    tiles = assemble(pieces)
    own_b = total(parts_b)
    own_a = total(parts_a)
    rounded_b = spread(own_b, "gy")
    rounded_a = spread(own_a, "gz")
    out_b = product_two(True, columns, rounded_b, tiles, here)
    crossed = scatter(out_b, "gy")
    picked = pick(crossed)
    got_b = scatter(picked, "gz")
    out_a = product_two(False, inverse, rounded_a, tiles, here)
    got_a = scatter(out_a, "gy")
    return finish(got_a, got_b, here)


def solution(mesh):
    in_specs = (P("gy", "gx", "gz", None, None, None), P("gy", "gx", "gz", None))
    out_specs = P(("gx", "gy"), "gz")
    return jax.shard_map(local, mesh=mesh, in_specs=in_specs, out_specs=out_specs, check_vma=False)
```

```python
import functools

import jax
import jax.numpy as jnp
from jax import lax
from jax.experimental import pallas as pl
from jax.experimental.pallas import tpu as pltpu
from jax.sharding import PartitionSpec as P

WIN = 1
UNROLL = 32
VMEM = pltpu.MemorySpace.VMEM
SMEM = pltpu.MemorySpace.SMEM


def limit(mib):
    return pltpu.CompilerParams(vmem_limit_bytes=mib << 20)


def assemble_kernel(parts, *refs):
    part_refs, out_ref, sems = refs[:parts], refs[parts], refs[parts + 1]
    here = part_refs[0].shape[0]
    copies = [
        pltpu.make_async_copy(part_refs[t], out_ref.at[pl.ds(t * here, here)], sems.at[t])
        for t in range(parts)
    ]
    for copy in copies:
        copy.start()
    for copy in copies:
        copy.wait()


def assemble(parts):
    here = parts[0].shape[0]
    shape = (here * len(parts),) + parts[0].shape[1:]
    return pl.pallas_call(
        functools.partial(assemble_kernel, len(parts)),
        out_shape=pltpu.VMEM(shape, jnp.bfloat16),
        in_specs=[pl.BlockSpec(memory_space=pltpu.HBM)] * len(parts),
        out_specs=pl.BlockSpec(memory_space=VMEM),
        scratch_shapes=[pltpu.SemaphoreType.DMA((len(parts),))],
        compiler_params=limit(46),
        cost_estimate=pl.CostEstimate(flops=4_000_000, bytes_accessed=25_000_000, transcendentals=0),
        name="assemble",
    )(*parts)


def pick_kernel(*refs):
    blocks = len(refs) // 2
    a, b = lax.axis_index("gy"), lax.axis_index("gz")
    for m in range(blocks):
        for k in range(blocks):

            @pl.when(a ^ b ^ k == m)
            def _(k=k, m=m):
                refs[blocks + k][...] = refs[m][...]


def pick(values):
    return pl.pallas_call(
        pick_kernel,
        out_shape=[jax.ShapeDtypeStruct(value.shape, value.dtype) for value in values],
        in_specs=[pl.BlockSpec(memory_space=VMEM)] * len(values),
        out_specs=[pl.BlockSpec(memory_space=VMEM)] * len(values),
        compiler_params=limit(8),
        cost_estimate=pl.CostEstimate(flops=1_000_000, bytes_accessed=2_000_000, transcendentals=0),
        name="pick",
    )(*values)


def swaps(size, step):
    return [(i, i ^ step) for i in range(size)]


def invert_kernel(cols_ref, inv_ref):
    rows, slots = cols_ref.shape
    count = rows * slots
    lane = lax.broadcasted_iota(jnp.int32, (rows, 128), 1)
    hits = jnp.concatenate(
        [(cols_ref[:, j : j + 1] == lane).astype(jnp.float32) for j in range(slots)], axis=0
    )
    above = lax.broadcasted_iota(jnp.int32, (count, count), 0) > lax.broadcasted_iota(
        jnp.int32, (count, count), 1
    )
    rank = jnp.dot(
        above.astype(jnp.bfloat16), hits.astype(jnp.bfloat16), preferred_element_type=jnp.float32
    )
    code = jnp.concatenate(
        [lax.broadcasted_iota(jnp.int32, (rows, 128), 0) * 8 + j for j in range(slots)], axis=0
    ).astype(jnp.float32)
    code = code * hits
    lines = [
        jnp.sum(jnp.where(rank == n, code, 0.0), axis=0, keepdims=True) for n in range(slots)
    ]
    lines += [jnp.zeros_like(lines[0])] * (8 - slots)
    inv_ref[...] = jnp.concatenate(lines, axis=0).astype(jnp.int32)


def invert(columns):
    return pl.pallas_call(
        invert_kernel,
        out_shape=jax.ShapeDtypeStruct((8, 128), jnp.int32),
        in_specs=[pl.BlockSpec(memory_space=VMEM)],
        out_specs=pl.BlockSpec(memory_space=VMEM),
        compiler_params=limit(4),
        cost_estimate=pl.CostEstimate(flops=4_000_000, bytes_accessed=4096, transcendentals=0),
        name="invert",
    )(columns)


def product_one_kernel(by_rows, lefts, parts, index_ref, *refs):
    left_refs, refs = refs[:lefts], refs[lefts:]
    part_refs, refs = refs[:parts], refs[parts:]
    blocks = len(refs) - 4
    send_refs, (left_ref, tile_ref, product_ref, sems) = refs[:blocks], refs[blocks:]
    g, a, b = lax.axis_index("gx"), lax.axis_index("gy"), lax.axis_index("gz")
    here, slots = part_refs[0].shape[:2]
    slab = here * parts
    rows = product_ref.shape[2]
    height = blocks * rows
    chosen = a ^ b if by_rows else a
    for k in range(lefts):

        @pl.when(chosen == k)
        def _(k=k):
            left_ref[...] = left_refs[k][...]

    tail = left_ref[pl.ds(slots * height, 16), :].astype(jnp.float32)
    columns = [jnp.max(tail[k : k + 1, :]).astype(jnp.int32) for k in range(slots)]
    targets = []
    for k in range(slots):
        if by_rows:
            p = lax.rem(columns[k] + slab - here * g, slab)
            targets.append([index_ref[p, j] for j in range(slots)])
            for t in range(parts):

                @pl.when(p // here == t)
                def _(k=k, t=t, p=p):
                    pltpu.make_async_copy(
                        part_refs[t].at[lax.rem(p, here)], tile_ref.at[k], sems.at[k, 0]
                    ).start()

        else:
            entries = [index_ref[n, columns[k]] for n in range(slots)]
            targets.append([entry >> 3 for entry in entries])
            for n in range(slots):
                p, j = entries[n] >> 3, entries[n] & 7
                for t in range(parts):

                    @pl.when(p // here == t)
                    def _(k=k, n=n, t=t, p=p, j=j):
                        pltpu.make_async_copy(
                            part_refs[t].at[lax.rem(p, here), j], tile_ref.at[k, n], sems.at[k, n]
                        ).start()

    lane = lax.broadcasted_iota(jnp.int32, (rows, left_ref.shape[1]), 1)
    places = jnp.zeros_like(lane)
    for k in range(slots):
        left = left_ref[pl.ds(k * height, height), :]
        if by_rows:
            pltpu.make_async_copy(part_refs[0].at[0], tile_ref.at[k], sems.at[k, 0]).wait()
        else:
            for n in range(slots):
                pltpu.make_async_copy(part_refs[0].at[0, 0], tile_ref.at[k, n], sems.at[k, n]).wait()
        for n in range(slots):
            product = lax.dot_general(
                left,
                tile_ref[k, n],
                (((1,), (0 if by_rows else 1,)), ((), ())),
                preferred_element_type=jnp.float32,
            ).astype(jnp.bfloat16)
            places = jnp.where(lane == k * slots + n, targets[k][n], places)
            for q in range(blocks):
                product_ref[q, k * slots + n] = product[q * rows : (q + 1) * rows]
    places = places.astype(jnp.float32).astype(jnp.bfloat16)
    me = a if by_rows else b
    for k in range(blocks):
        send_refs[k][pl.ds(0, slots * slots)] = product_ref[me ^ k]
        send_refs[k][slots * slots] = places


def product_one(by_rows, index, lefts, parts, blocks, height):
    slots, tile = parts[0].shape[1:3]
    rows = height // blocks
    message = jax.ShapeDtypeStruct((slots * slots + 1, rows, tile), jnp.bfloat16)
    return pl.pallas_call(
        functools.partial(product_one_kernel, by_rows, len(lefts), len(parts)),
        out_shape=[message] * blocks,
        in_specs=[pl.BlockSpec(memory_space=SMEM)]
        + [pl.BlockSpec(memory_space=VMEM)] * len(lefts)
        + [pl.BlockSpec(memory_space=pltpu.HBM)] * len(parts),
        out_specs=[pl.BlockSpec(memory_space=VMEM)] * blocks,
        scratch_shapes=[
            pltpu.VMEM(lefts[0].shape, jnp.bfloat16),
            pltpu.VMEM((slots, slots, tile, tile), jnp.bfloat16),
            pltpu.VMEM((blocks, slots * slots, rows, tile), jnp.bfloat16),
            pltpu.SemaphoreType.DMA((slots, slots)),
        ],
        compiler_params=limit(50),
        cost_estimate=pl.CostEstimate(flops=12_000_000, bytes_accessed=4_000_000, transcendentals=0),
        name="one_rows" if by_rows else "one_columns",
    )(index, *lefts, *parts)


def merge_kernel(*refs):
    sources = len(refs) - 5
    message_refs, (out_ref, acc_ref, vector_ref, place_ref, sem) = refs[:sources], refs[sources:]
    count = message_refs[0].shape[0] - 1
    lines = [ref[count].astype(jnp.float32)[0:1] for ref in message_refs]
    lines += [jnp.zeros_like(lines[0])] * (8 - sources)
    vector_ref[...] = jnp.concatenate(lines, axis=0).astype(jnp.int32)
    copy = pltpu.make_async_copy(vector_ref, place_ref, sem)
    copy.start()
    acc_ref[...] = jnp.zeros_like(acc_ref)
    copy.wait()
    for e in range(count):
        for s in range(sources):
            acc_ref[place_ref[s, e]] += message_refs[s][e].astype(jnp.float32)
    out_ref[...] = acc_ref[...].astype(jnp.bfloat16)


def merge(messages, slab):
    _, rows, tile = messages[0].shape
    return pl.pallas_call(
        merge_kernel,
        out_shape=jax.ShapeDtypeStruct((slab, rows, tile), jnp.bfloat16),
        in_specs=[pl.BlockSpec(memory_space=VMEM)] * len(messages),
        out_specs=pl.BlockSpec(memory_space=VMEM),
        scratch_shapes=[
            pltpu.VMEM((slab, rows, tile), jnp.float32),
            pltpu.VMEM((8, 128), jnp.int32),
            pltpu.SMEM((8, 128), jnp.int32),
            pltpu.SemaphoreType.DMA,
        ],
        compiler_params=limit(8),
        cost_estimate=pl.CostEstimate(flops=4_000_000, bytes_accessed=1_000_000, transcendentals=0),
        name="merge",
    )(*messages)


def product_two_kernel(by_rows, here, blocks, index_ref, slab_ref, *refs):
    round_refs, refs = refs[:blocks], refs[blocks:]
    send_refs, (left_ref,) = refs[:blocks], refs[blocks:]
    g, a, b = lax.axis_index("gx"), lax.axis_index("gy"), lax.axis_index("gz")
    slab, slots = slab_ref.shape[:2]
    rows = left_ref.shape[2]
    for k in range(blocks):
        left_ref[k if by_rows else a ^ b ^ k] = round_refs[k][...]
    extra = jnp.where(a == b, 3.0, 0.0).astype(jnp.float32)

    def left_of(p):
        return jnp.concatenate([left_ref[m, p] for m in range(blocks)], axis=0)

    def one(q, lefts, tiles, same):
        summed = None
        for n in range(0, slots, 2):
            left = jnp.concatenate([left_of(p) for p in lefts[n : n + 2]], axis=1)
            pair = jnp.concatenate(tiles[n : n + 2], axis=1 if by_rows else 0)
            if by_rows:
                first, second, contract = pair, left, 1
            else:
                first, second, contract = left, pair, 0
            product = lax.dot_general(
                first,
                second,
                (((1,), (contract,)), ((), ())),
                preferred_element_type=jnp.float32,
            )
            summed = product if summed is None else summed + product
        summed = summed.T if by_rows else summed
        for m in range(blocks):
            value = extra * left_ref[m, same].astype(jnp.float32) - 2.0 * summed[m * rows : (m + 1) * rows]
            send_refs[m][q] = value.astype(jnp.bfloat16)

    @pl.loop(0, slab, step=UNROLL)
    def _(first):
        for u in range(UNROLL):
            q = first + u
            entries = [index_ref[q, n] if by_rows else index_ref[n, q] for n in range(slots)]
            if by_rows:
                tiles = [slab_ref[q, j] for j in range(slots)]
                one(q, entries, tiles, lax.rem(q + here * g, slab))
            else:
                lefts = [entry >> 3 for entry in entries]
                tiles = [slab_ref[entry >> 3, entry & 7] for entry in entries]
                one(q, lefts, tiles, lax.rem(q + slab - here * g, slab))


def product_two(by_rows, index, rounded, tiles, here):
    slab, _, tile = tiles.shape[:3]
    blocks = len(rounded)
    rows = rounded[0].shape[1]
    message = jax.ShapeDtypeStruct((slab, rows, tile), jnp.bfloat16)
    return pl.pallas_call(
        functools.partial(product_two_kernel, by_rows, here, blocks),
        out_shape=[message] * blocks,
        in_specs=[pl.BlockSpec(memory_space=SMEM)]
        + [pl.BlockSpec(memory_space=VMEM)] * (1 + blocks),
        out_specs=[pl.BlockSpec(memory_space=VMEM)] * blocks,
        scratch_shapes=[pltpu.VMEM((blocks, slab, rows, tile), jnp.bfloat16)],
        compiler_params=limit(20),
        cost_estimate=pl.CostEstimate(flops=30_000_000, bytes_accessed=12_000_000, transcendentals=0),
        name="two_rows" if by_rows else "two_columns",
    )(index, tiles, *rounded)


def finish_kernel(here, *refs):
    half = len(refs) // 2
    first, second, out_ref = refs[:half], refs[half:-1], refs[-1]
    g = lax.axis_index("gx")
    slab, rows, tile = first[0].shape

    def add(refs_in, y):
        total = refs_in[0][y].astype(jnp.float32)
        for ref in refs_in[1:]:
            total = total + ref[y].astype(jnp.float32)
        return total

    @pl.loop(0, slab, unroll=8)
    def _(y):
        columns = pl.ds(pl.multiple_of(y * tile, tile), tile)
        out_ref[0:rows, columns] = add(first, y)
        out_ref[rows : 2 * rows, columns] = add(second, lax.rem(y + slab - here * g, slab))


def finish(first, second, here):
    slab, rows, tile = first[0].shape
    return pl.pallas_call(
        functools.partial(finish_kernel, here),
        out_shape=jax.ShapeDtypeStruct((2 * rows, slab * tile), jnp.float32),
        in_specs=[pl.BlockSpec(memory_space=VMEM)] * (len(first) + len(second)),
        out_specs=pl.BlockSpec(memory_space=VMEM),
        compiler_params=limit(8),
        name="finish",
    )(*first, *second)


def local(block_values, block_cols):
    tiles_here = block_values[0, :, 0]
    columns_here = block_cols[0, :, 0]
    here, slots, tile, _ = tiles_here.shape
    parts = lax.axis_size("gx")
    size = lax.axis_size("gy")
    blocks = WIN * tile // size
    rows = blocks // 2
    height = rows * size

    def payload(first):
        window = tiles_here[0].reshape(slots, size, blocks, tile)[:, :, first : first + rows]
        tail = jnp.broadcast_to(columns_here[0].astype(jnp.bfloat16)[:, None], (slots, tile))
        tail = jnp.pad(tail, ((0, 16 - slots), (0, 0)))
        return jnp.concatenate([window.reshape(slots * height, tile), tail], axis=0)

    pay_a, pay_b = payload(0), payload(rows)
    both = ("gy", "gz")
    shifts = [[((i + t) % parts, i) for i in range(parts)] for t in range(1, parts)]
    others = [lax.ppermute(columns_here, "gx", s) for s in shifts]
    moved = [lax.ppermute(tiles_here, "gx", s) for s in shifts]
    left_b = [
        lax.ppermute(pay_b, both, [(a, a * size + (a ^ k)) for a in range(size)]) for k in range(size)
    ]
    left_a = [pay_a] + [lax.ppermute(pay_a, "gy", [(0, k)]) for k in range(1, size)]
    columns = jnp.concatenate([columns_here] + others, axis=0)
    inverse = invert(columns)
    pieces = [tiles_here] + moved

    def scatter(sends, axis):
        return [sends[0]] + [lax.ppermute(sends[k], axis, swaps(size, k)) for k in range(1, size)]

    def spread(own, axis):
        return [own] + [lax.ppermute(own, axis, swaps(size, k)) for k in range(1, size)]

    sends_a = product_one(False, inverse, left_a, pieces, size, height)
    parts_a = scatter(sends_a, "gz")
    _, left_b = lax.optimization_barrier((sends_a[0], left_b))
    sends_b = product_one(True, columns, left_b, pieces, size, height)
    parts_b = scatter(sends_b, "gy")
    tiles = assemble(pieces)
    own_b = merge(parts_b, here * parts)
    own_a = merge(parts_a, here * parts)
    rounded_b = spread(own_b, "gy")
    rounded_a = spread(own_a, "gz")
    out_b = product_two(True, columns, rounded_b, tiles, here)
    crossed = scatter(out_b, "gy")
    picked = pick(crossed)
    got_b = scatter(picked, "gz")
    out_a = product_two(False, inverse, rounded_a, tiles, here)
    got_a = scatter(out_a, "gy")
    return finish(got_a, got_b, here)


def solution(mesh):
    in_specs = (P("gy", "gx", "gz", None, None, None), P("gy", "gx", "gz", None))
    out_specs = P(("gx", "gy"), "gz")
    return jax.shard_map(local, mesh=mesh, in_specs=in_specs, out_specs=out_specs, check_vma=False)
```

```python
import functools
import math

import jax
import jax.numpy as jnp
from jax import lax
from jax.experimental import pallas as pl
from jax.experimental.pallas import tpu as pltpu
from jax.sharding import PartitionSpec as P

WIN = 1
UNROLL = 64
VMEM = pltpu.MemorySpace.VMEM
SMEM = pltpu.MemorySpace.SMEM


def limit(mib):
    return pltpu.CompilerParams(vmem_limit_bytes=mib << 20)


def assemble_kernel(parts, *refs):
    part_refs, out_ref, sems = refs[:parts], refs[parts], refs[parts + 1]
    here = part_refs[0].shape[0]
    copies = [
        pltpu.make_async_copy(part_refs[t], out_ref.at[pl.ds(t * here, here)], sems.at[t])
        for t in range(parts)
    ]
    for copy in copies:
        copy.start()
    for copy in copies:
        copy.wait()


def assemble(parts):
    here = parts[0].shape[0]
    shape = (here * len(parts),) + parts[0].shape[1:]
    return pl.pallas_call(
        functools.partial(assemble_kernel, len(parts)),
        out_shape=pltpu.VMEM(shape, jnp.bfloat16),
        in_specs=[pl.BlockSpec(memory_space=pltpu.HBM)] * len(parts),
        out_specs=pl.BlockSpec(memory_space=VMEM),
        scratch_shapes=[pltpu.SemaphoreType.DMA((len(parts),))],
        compiler_params=limit(46),
        cost_estimate=pl.CostEstimate(flops=4_000_000, bytes_accessed=25_000_000, transcendentals=0),
        name="assemble",
    )(*parts)


def pick_kernel(*refs):
    blocks = len(refs) // 2
    a, b = lax.axis_index("gy"), lax.axis_index("gz")
    for m in range(blocks):
        for k in range(blocks):

            @pl.when(a ^ b ^ k == m)
            def _(k=k, m=m):
                refs[blocks + k][...] = refs[m][...]


def pick(values):
    return pl.pallas_call(
        pick_kernel,
        out_shape=[jax.ShapeDtypeStruct(value.shape, value.dtype) for value in values],
        in_specs=[pl.BlockSpec(memory_space=VMEM)] * len(values),
        out_specs=[pl.BlockSpec(memory_space=VMEM)] * len(values),
        compiler_params=limit(8),
        cost_estimate=pl.CostEstimate(flops=1_000_000, bytes_accessed=2_000_000, transcendentals=0),
        name="pick",
    )(*values)


def swaps(size, step):
    return [(i, i ^ step) for i in range(size)]


def payload_kernel(tiles_ref, turned_ref, first_ref, second_ref, window_ref, sem):
    copy = pltpu.make_async_copy(tiles_ref.at[0], window_ref, sem)
    copy.start()
    slots, _ = window_ref.shape[:2]
    height = (first_ref.shape[0] - 16) // slots
    size = lax.axis_size("gy")
    rows = height // size
    tail = jnp.broadcast_to(turned_ref[:, 0:1].astype(jnp.float32), (slots, first_ref.shape[1]))
    tail = jnp.concatenate([tail, jnp.zeros((16 - slots, first_ref.shape[1]), jnp.float32)], axis=0)
    tail = tail.astype(jnp.bfloat16)
    copy.wait()
    for half, ref in enumerate((first_ref, second_ref)):
        for k in range(slots):
            for r in range(size):
                start = (2 * r + half) * rows
                ref[k * height + r * rows : k * height + (r + 1) * rows] = window_ref[k, start : start + rows]
        ref[slots * height :] = tail


def payloads(tiles, columns, height):
    slots, tile = tiles.shape[1:3]
    shape = jax.ShapeDtypeStruct((slots * height + 16, tile), jnp.bfloat16)
    return pl.pallas_call(
        payload_kernel,
        out_shape=[shape] * 2,
        in_specs=[pl.BlockSpec(memory_space=pltpu.HBM), pl.BlockSpec(memory_space=VMEM)],
        out_specs=[pl.BlockSpec(memory_space=VMEM)] * 2,
        scratch_shapes=[pltpu.VMEM(tiles.shape[1:], jnp.bfloat16), pltpu.SemaphoreType.DMA],
        compiler_params=limit(50),
        cost_estimate=pl.CostEstimate(flops=1_000_000, bytes_accessed=400_000, transcendentals=0),
        name="payload",
    )(tiles, columns.T)


def invert_kernel(cols_ref, inv_ref):
    rows, slots = cols_ref.shape
    count = rows * slots
    lane = lax.broadcasted_iota(jnp.int32, (rows, 128), 1)
    hits = jnp.concatenate(
        [(cols_ref[:, j : j + 1] == lane).astype(jnp.float32) for j in range(slots)], axis=0
    )
    above = lax.broadcasted_iota(jnp.int32, (count, count), 0) > lax.broadcasted_iota(
        jnp.int32, (count, count), 1
    )
    rank = jnp.dot(
        above.astype(jnp.bfloat16), hits.astype(jnp.bfloat16), preferred_element_type=jnp.float32
    )
    code = jnp.concatenate(
        [lax.broadcasted_iota(jnp.int32, (rows, 128), 0) * 8 + j for j in range(slots)], axis=0
    ).astype(jnp.float32)
    code = code * hits
    lines = [
        jnp.sum(jnp.where(rank == n, code, 0.0), axis=0, keepdims=True) for n in range(slots)
    ]
    lines += [jnp.zeros_like(lines[0])] * (8 - slots)
    inv_ref[...] = jnp.concatenate(lines, axis=0).astype(jnp.int32)


def invert(columns):
    return pl.pallas_call(
        invert_kernel,
        out_shape=jax.ShapeDtypeStruct((8, 128), jnp.int32),
        in_specs=[pl.BlockSpec(memory_space=VMEM)],
        out_specs=pl.BlockSpec(memory_space=VMEM),
        compiler_params=limit(4),
        cost_estimate=pl.CostEstimate(flops=4_000_000, bytes_accessed=4096, transcendentals=0),
        name="invert",
    )(columns)


def product_one_kernel(by_rows, lefts, parts, index_ref, *refs):
    left_refs, refs = refs[:lefts], refs[lefts:]
    part_refs, refs = refs[:parts], refs[parts:]
    blocks = len(refs) - 4
    send_refs, (left_ref, tile_ref, product_ref, sems) = refs[:blocks], refs[blocks:]
    g, a, b = lax.axis_index("gx"), lax.axis_index("gy"), lax.axis_index("gz")
    here, slots = part_refs[0].shape[:2]
    slab = here * parts
    rows = product_ref.shape[2]
    height = blocks * rows
    chosen = a ^ b if by_rows else a
    for k in range(lefts):

        @pl.when(chosen == k)
        def _(k=k):
            left_ref[pl.ds(slots * height, 16)] = left_refs[k][pl.ds(slots * height, 16)]

    tail = left_ref[pl.ds(slots * height, 16), :].astype(jnp.float32)
    columns = [jnp.max(tail[k : k + 1, :]).astype(jnp.int32) for k in range(slots)]
    targets = []
    for k in range(slots):
        if by_rows:
            p = lax.rem(columns[k] + slab - here * g, slab)
            targets.append([index_ref[p, j] for j in range(slots)])
            for t in range(parts):

                @pl.when(p // here == t)
                def _(k=k, t=t, p=p):
                    pltpu.make_async_copy(
                        part_refs[t].at[lax.rem(p, here)], tile_ref.at[k], sems.at[k, 0]
                    ).start()

        else:
            entries = [index_ref[n, columns[k]] for n in range(slots)]
            targets.append([entry >> 3 for entry in entries])
            for n in range(slots):
                p, j = entries[n] >> 3, entries[n] & 7
                for t in range(parts):

                    @pl.when(p // here == t)
                    def _(k=k, n=n, t=t, p=p, j=j):
                        pltpu.make_async_copy(
                            part_refs[t].at[lax.rem(p, here), j], tile_ref.at[k, n], sems.at[k, n]
                        ).start()

    for k in range(lefts):

        @pl.when(chosen == k)
        def _(k=k):
            left_ref[pl.ds(0, slots * height)] = left_refs[k][pl.ds(0, slots * height)]

    lane = lax.broadcasted_iota(jnp.int32, (rows, left_ref.shape[1]), 1)
    places = jnp.zeros_like(lane)
    for k in range(slots):
        left = left_ref[pl.ds(k * height, height), :]
        if by_rows:
            pltpu.make_async_copy(part_refs[0].at[0], tile_ref.at[k], sems.at[k, 0]).wait()
        else:
            for n in range(slots):
                pltpu.make_async_copy(part_refs[0].at[0, 0], tile_ref.at[k, n], sems.at[k, n]).wait()
        for n in range(slots):
            product = lax.dot_general(
                left,
                tile_ref[k, n],
                (((1,), (0 if by_rows else 1,)), ((), ())),
                preferred_element_type=jnp.float32,
            ).astype(jnp.bfloat16)
            places = jnp.where(lane == k * slots + n, targets[k][n], places)
            for q in range(blocks):
                product_ref[q, k * slots + n] = product[q * rows : (q + 1) * rows]
    places = places.astype(jnp.float32).astype(jnp.bfloat16)
    me = a if by_rows else b
    for k in range(blocks):
        send_refs[k][pl.ds(0, slots * slots)] = product_ref[me ^ k]
        send_refs[k][slots * slots] = places


def product_one(by_rows, index, lefts, parts, blocks, height):
    slots, tile = parts[0].shape[1:3]
    rows = height // blocks
    message = jax.ShapeDtypeStruct((slots * slots + 1, rows, tile), jnp.bfloat16)
    return pl.pallas_call(
        functools.partial(product_one_kernel, by_rows, len(lefts), len(parts)),
        out_shape=[message] * blocks,
        in_specs=[pl.BlockSpec(memory_space=SMEM)]
        + [pl.BlockSpec(memory_space=VMEM)] * len(lefts)
        + [pl.BlockSpec(memory_space=pltpu.HBM)] * len(parts),
        out_specs=[pl.BlockSpec(memory_space=VMEM)] * blocks,
        scratch_shapes=[
            pltpu.VMEM(lefts[0].shape, jnp.bfloat16),
            pltpu.VMEM((slots, slots, tile, tile), jnp.bfloat16),
            pltpu.VMEM((blocks, slots * slots, rows, tile), jnp.bfloat16),
            pltpu.SemaphoreType.DMA((slots, slots)),
        ],
        compiler_params=limit(50),
        cost_estimate=pl.CostEstimate(flops=12_000_000, bytes_accessed=4_000_000, transcendentals=0),
        name="one_rows" if by_rows else "one_columns",
    )(index, *lefts, *parts)


def merge_kernel(*refs):
    sources = len(refs) - 5
    message_refs, (out_ref, acc_ref, vector_ref, place_ref, sem) = refs[:sources], refs[sources:]
    count = message_refs[0].shape[0] - 1
    lines = [ref[count].astype(jnp.float32)[0:1] for ref in message_refs]
    lines += [jnp.zeros_like(lines[0])] * (8 - sources)
    vector_ref[...] = jnp.concatenate(lines, axis=0).astype(jnp.int32)
    copy = pltpu.make_async_copy(vector_ref, place_ref, sem)
    copy.start()
    acc_ref[...] = jnp.zeros_like(acc_ref)
    copy.wait()
    for e in range(count):
        for s in range(sources):
            acc_ref[place_ref[s, e]] += message_refs[s][e].astype(jnp.float32)
    out_ref[...] = acc_ref[...].astype(jnp.bfloat16)


def merge(messages, slab):
    _, rows, tile = messages[0].shape
    return pl.pallas_call(
        merge_kernel,
        out_shape=jax.ShapeDtypeStruct((slab, rows, tile), jnp.bfloat16),
        in_specs=[pl.BlockSpec(memory_space=VMEM)] * len(messages),
        out_specs=pl.BlockSpec(memory_space=VMEM),
        scratch_shapes=[
            pltpu.VMEM((slab, rows, tile), jnp.float32),
            pltpu.VMEM((8, 128), jnp.int32),
            pltpu.SMEM((8, 128), jnp.int32),
            pltpu.SemaphoreType.DMA,
        ],
        compiler_params=limit(8),
        cost_estimate=pl.CostEstimate(flops=4_000_000, bytes_accessed=1_000_000, transcendentals=0),
        name="merge",
    )(*messages)


def product_two_kernel(by_rows, here, blocks, index_ref, slab_ref, *refs):
    round_refs, refs = refs[:blocks], refs[blocks:]
    send_refs, (left_ref,) = refs[:blocks], refs[blocks:]
    g, a, b = lax.axis_index("gx"), lax.axis_index("gy"), lax.axis_index("gz")
    slab, slots = slab_ref.shape[:2]
    rows = left_ref.shape[2]
    for k in range(blocks):
        left_ref[k if by_rows else a ^ b ^ k] = round_refs[k][...]
    extra = jnp.where(a == b, 3.0, 0.0).astype(jnp.float32)

    def left_of(p):
        return jnp.concatenate([left_ref[m, p] for m in range(blocks)], axis=0)

    def one(q, lefts, tiles, same):
        summed = None
        for n in range(0, slots, 2):
            left = jnp.concatenate([left_of(p) for p in lefts[n : n + 2]], axis=1)
            pair = jnp.concatenate(tiles[n : n + 2], axis=1 if by_rows else 0)
            if by_rows:
                first, second, contract = pair, left, 1
            else:
                first, second, contract = left, pair, 0
            product = lax.dot_general(
                first,
                second,
                (((1,), (contract,)), ((), ())),
                preferred_element_type=jnp.float32,
            )
            summed = product if summed is None else summed + product
        summed = summed.T if by_rows else summed
        for m in range(blocks):
            value = extra * left_ref[m, same].astype(jnp.float32) - 2.0 * summed[m * rows : (m + 1) * rows]
            send_refs[m][q] = value.astype(jnp.bfloat16)

    unroll = math.gcd(UNROLL, slab)

    @pl.loop(0, slab, step=unroll)
    def _(first):
        for u in range(unroll):
            q = first + u
            entries = [index_ref[q, n] if by_rows else index_ref[n, q] for n in range(slots)]
            if by_rows:
                tiles = [slab_ref[q, j] for j in range(slots)]
                one(q, entries, tiles, lax.rem(q + here * g, slab))
            else:
                lefts = [entry >> 3 for entry in entries]
                tiles = [slab_ref[entry >> 3, entry & 7] for entry in entries]
                one(q, lefts, tiles, lax.rem(q + slab - here * g, slab))


def product_two(by_rows, index, rounded, tiles, here):
    slab, _, tile = tiles.shape[:3]
    blocks = len(rounded)
    rows = rounded[0].shape[1]
    message = jax.ShapeDtypeStruct((slab, rows, tile), jnp.bfloat16)
    return pl.pallas_call(
        functools.partial(product_two_kernel, by_rows, here, blocks),
        out_shape=[message] * blocks,
        in_specs=[pl.BlockSpec(memory_space=SMEM)]
        + [pl.BlockSpec(memory_space=VMEM)] * (1 + blocks),
        out_specs=[pl.BlockSpec(memory_space=VMEM)] * blocks,
        scratch_shapes=[pltpu.VMEM((blocks, slab, rows, tile), jnp.bfloat16)],
        compiler_params=limit(20),
        cost_estimate=pl.CostEstimate(flops=30_000_000, bytes_accessed=12_000_000, transcendentals=0),
        name="two_rows" if by_rows else "two_columns",
    )(index, tiles, *rounded)


def finish_kernel(here, *refs):
    half = len(refs) // 2
    first, second, out_ref = refs[:half], refs[half:-1], refs[-1]
    g = lax.axis_index("gx")
    slab, rows, tile = first[0].shape

    def add(refs_in, y):
        total = refs_in[0][y].astype(jnp.float32)
        for ref in refs_in[1:]:
            total = total + ref[y].astype(jnp.float32)
        return total

    @pl.loop(0, slab, unroll=8)
    def _(y):
        columns = pl.ds(pl.multiple_of(y * tile, tile), tile)
        out_ref[0:rows, columns] = add(first, y)
        out_ref[rows : 2 * rows, columns] = add(second, lax.rem(y + slab - here * g, slab))


def finish(first, second, here):
    slab, rows, tile = first[0].shape
    return pl.pallas_call(
        functools.partial(finish_kernel, here),
        out_shape=jax.ShapeDtypeStruct((2 * rows, slab * tile), jnp.float32),
        in_specs=[pl.BlockSpec(memory_space=VMEM)] * (len(first) + len(second)),
        out_specs=pl.BlockSpec(memory_space=VMEM),
        compiler_params=limit(8),
        name="finish",
    )(*first, *second)


def local(block_values, block_cols):
    tiles_here = block_values[0, :, 0]
    columns_here = block_cols[0, :, 0]
    here, _, tile, _ = tiles_here.shape
    parts = lax.axis_size("gx")
    size = lax.axis_size("gy")
    blocks = WIN * tile // size
    rows = blocks // 2
    height = rows * size

    pay_a, pay_b = payloads(tiles_here, columns_here, height)
    both = ("gy", "gz")
    shifts = [[((i + t) % parts, i) for i in range(parts)] for t in range(1, parts)]
    others = [lax.ppermute(columns_here, "gx", s) for s in shifts]
    moved = [lax.ppermute(tiles_here, "gx", s) for s in shifts]
    left_b = []
    for k in range(size):
        left_b.append(lax.ppermute(pay_b, both, [(a, a * size + (a ^ k)) for a in range(size)]))
    left_a = [pay_a]
    for k in range(1, size):
        left_a.append(lax.ppermute(pay_a, "gy", [(0, k)]))
    columns = jnp.concatenate([columns_here] + others, axis=0)
    inverse = invert(columns)
    pieces = [tiles_here] + moved

    def scatter(sends, axis):
        received = [sends[0]]
        for k in range(1, size):
            received.append(lax.ppermute(sends[k], axis, swaps(size, k)))
        return received

    def spread(own, axis):
        return scatter([own] * size, axis)

    sends_a = product_one(False, inverse, left_a, pieces, size, height)
    parts_a = scatter(sends_a, "gz")
    _, left_b = lax.optimization_barrier((sends_a[0], left_b))
    sends_b = product_one(True, columns, left_b, pieces, size, height)
    parts_b = scatter(sends_b, "gy")
    tiles = assemble(pieces)
    own_b = merge(parts_b, here * parts)
    own_a = merge(parts_a, here * parts)
    rounded_b = spread(own_b, "gy")
    rounded_a = spread(own_a, "gz")
    out_b = product_two(True, columns, rounded_b, tiles, here)
    crossed = scatter(out_b, "gy")
    picked = pick(crossed)
    got_b = scatter(picked, "gz")
    out_a = product_two(False, inverse, rounded_a, tiles, here)
    got_a = scatter(out_a, "gy")
    return finish(got_a, got_b, here)


def solution(mesh):
    in_specs = (P("gy", "gx", "gz", None, None, None), P("gy", "gx", "gz", None))
    out_specs = P(("gx", "gy"), "gz")
    return jax.shard_map(local, mesh=mesh, in_specs=in_specs, out_specs=out_specs, check_vma=False)
```

```python
import functools
import math

import jax
import jax.numpy as jnp
from jax import lax
from jax.experimental import pallas as pl
from jax.experimental.pallas import tpu as pltpu
from jax.sharding import PartitionSpec as P

WIN = 1
UNROLL = 64
VMEM = pltpu.MemorySpace.VMEM
SMEM = pltpu.MemorySpace.SMEM


def limit(mib):
    return pltpu.CompilerParams(vmem_limit_bytes=mib << 20)


def assemble_kernel(parts, *refs):
    part_refs, out_ref, sems = refs[:parts], refs[parts], refs[parts + 1]
    here = part_refs[0].shape[0]
    copies = [
        pltpu.make_async_copy(part_refs[t], out_ref.at[pl.ds(t * here, here)], sems.at[t])
        for t in range(parts)
    ]
    for copy in copies:
        copy.start()
    for copy in copies:
        copy.wait()


def assemble(parts):
    here = parts[0].shape[0]
    shape = (here * len(parts),) + parts[0].shape[1:]
    return pl.pallas_call(
        functools.partial(assemble_kernel, len(parts)),
        out_shape=pltpu.VMEM(shape, jnp.bfloat16),
        in_specs=[pl.BlockSpec(memory_space=pltpu.HBM)] * len(parts),
        out_specs=pl.BlockSpec(memory_space=VMEM),
        scratch_shapes=[pltpu.SemaphoreType.DMA((len(parts),))],
        compiler_params=limit(46),
        cost_estimate=pl.CostEstimate(flops=4_000_000, bytes_accessed=25_000_000, transcendentals=0),
        name="assemble",
    )(*parts)


def pick_kernel(*refs):
    blocks = len(refs) // 2
    a, b = lax.axis_index("gy"), lax.axis_index("gz")
    for m in range(blocks):
        for k in range(blocks):

            @pl.when(a ^ b ^ k == m)
            def _(k=k, m=m):
                refs[blocks + k][...] = refs[m][...]


def pick(values):
    return pl.pallas_call(
        pick_kernel,
        out_shape=[jax.ShapeDtypeStruct(value.shape, value.dtype) for value in values],
        in_specs=[pl.BlockSpec(memory_space=VMEM)] * len(values),
        out_specs=[pl.BlockSpec(memory_space=VMEM)] * len(values),
        compiler_params=limit(8),
        cost_estimate=pl.CostEstimate(flops=1_000_000, bytes_accessed=2_000_000, transcendentals=0),
        name="pick",
    )(*values)


def swaps(size, step):
    return [(i, i ^ step) for i in range(size)]


def payload_kernel(tiles_ref, turned_ref, first_ref, second_ref, window_ref, sem):
    copy = pltpu.make_async_copy(tiles_ref.at[0], window_ref, sem)
    copy.start()
    slots, _ = window_ref.shape[:2]
    height = (first_ref.shape[0] - 16) // slots
    size = lax.axis_size("gy")
    rows = height // size
    tail = jnp.broadcast_to(turned_ref[:, 0:1].astype(jnp.float32), (slots, first_ref.shape[1]))
    tail = jnp.concatenate([tail, jnp.zeros((16 - slots, first_ref.shape[1]), jnp.float32)], axis=0)
    tail = tail.astype(jnp.bfloat16)
    copy.wait()
    for half, ref in enumerate((first_ref, second_ref)):
        for k in range(slots):
            for r in range(size):
                start = (2 * r + half) * rows
                ref[k * height + r * rows : k * height + (r + 1) * rows] = window_ref[k, start : start + rows]
        ref[slots * height :] = tail


def payloads(tiles, columns, height):
    slots, tile = tiles.shape[1:3]
    shape = jax.ShapeDtypeStruct((slots * height + 16, tile), jnp.bfloat16)
    return pl.pallas_call(
        payload_kernel,
        out_shape=[shape] * 2,
        in_specs=[pl.BlockSpec(memory_space=pltpu.HBM), pl.BlockSpec(memory_space=VMEM)],
        out_specs=[pl.BlockSpec(memory_space=VMEM)] * 2,
        scratch_shapes=[pltpu.VMEM(tiles.shape[1:], jnp.bfloat16), pltpu.SemaphoreType.DMA],
        compiler_params=limit(50),
        cost_estimate=pl.CostEstimate(flops=1_000_000, bytes_accessed=400_000, transcendentals=0),
        name="payload",
    )(tiles, columns.T)


def invert_kernel(cols_ref, inv_ref):
    rows, slots = cols_ref.shape
    count = rows * slots
    lane = lax.broadcasted_iota(jnp.int32, (rows, 128), 1)
    hits = jnp.concatenate(
        [(cols_ref[:, j : j + 1] == lane).astype(jnp.float32) for j in range(slots)], axis=0
    )
    above = lax.broadcasted_iota(jnp.int32, (count, count), 0) > lax.broadcasted_iota(
        jnp.int32, (count, count), 1
    )
    rank = jnp.dot(
        above.astype(jnp.bfloat16), hits.astype(jnp.bfloat16), preferred_element_type=jnp.float32
    )
    code = jnp.concatenate(
        [lax.broadcasted_iota(jnp.int32, (rows, 128), 0) * 8 + j for j in range(slots)], axis=0
    ).astype(jnp.float32)
    code = code * hits
    lines = [
        jnp.sum(jnp.where(rank == n, code, 0.0), axis=0, keepdims=True) for n in range(slots)
    ]
    lines += [jnp.zeros_like(lines[0])] * (8 - slots)
    inv_ref[...] = jnp.concatenate(lines, axis=0).astype(jnp.int32)


def invert(columns):
    return pl.pallas_call(
        invert_kernel,
        out_shape=jax.ShapeDtypeStruct((8, 128), jnp.int32),
        in_specs=[pl.BlockSpec(memory_space=VMEM)],
        out_specs=pl.BlockSpec(memory_space=VMEM),
        compiler_params=limit(4),
        cost_estimate=pl.CostEstimate(flops=4_000_000, bytes_accessed=4096, transcendentals=0),
        name="invert",
    )(columns)


def product_one_kernel(by_rows, lefts, parts, index_ref, *refs):
    left_refs, refs = refs[:lefts], refs[lefts:]
    part_refs, refs = refs[:parts], refs[parts:]
    blocks = len(refs) - 4
    send_refs, (left_ref, tile_ref, product_ref, sems) = refs[:blocks], refs[blocks:]
    g, a, b = lax.axis_index("gx"), lax.axis_index("gy"), lax.axis_index("gz")
    here, slots = part_refs[0].shape[:2]
    slab = here * parts
    rows = product_ref.shape[2]
    height = blocks * rows
    chosen = a ^ b if by_rows else a
    for k in range(lefts):

        @pl.when(chosen == k)
        def _(k=k):
            left_ref[pl.ds(slots * height, 16)] = left_refs[k][pl.ds(slots * height, 16)]

    tail = left_ref[pl.ds(slots * height, 16), :].astype(jnp.float32)
    columns = [jnp.max(tail[k : k + 1, :]).astype(jnp.int32) for k in range(slots)]
    targets = []
    for k in range(slots):
        if by_rows:
            p = lax.rem(columns[k] + slab - here * g, slab)
            targets.append([index_ref[p, j] for j in range(slots)])
            for t in range(parts):

                @pl.when(p // here == t)
                def _(k=k, t=t, p=p):
                    pltpu.make_async_copy(
                        part_refs[t].at[lax.rem(p, here)], tile_ref.at[k], sems.at[k, 0]
                    ).start()

        else:
            entries = [index_ref[n, columns[k]] for n in range(slots)]
            targets.append([entry >> 3 for entry in entries])
            for n in range(slots):
                p, j = entries[n] >> 3, entries[n] & 7
                for t in range(parts):

                    @pl.when(p // here == t)
                    def _(k=k, n=n, t=t, p=p, j=j):
                        pltpu.make_async_copy(
                            part_refs[t].at[lax.rem(p, here), j], tile_ref.at[k, n], sems.at[k, n]
                        ).start()

    for k in range(lefts):

        @pl.when(chosen == k)
        def _(k=k):
            left_ref[pl.ds(0, slots * height)] = left_refs[k][pl.ds(0, slots * height)]

    lane = lax.broadcasted_iota(jnp.int32, (rows, left_ref.shape[1]), 1)
    places = jnp.zeros_like(lane)
    for k in range(slots):
        left = left_ref[pl.ds(k * height, height), :]
        if by_rows:
            pltpu.make_async_copy(part_refs[0].at[0], tile_ref.at[k], sems.at[k, 0]).wait()
        else:
            for n in range(slots):
                pltpu.make_async_copy(part_refs[0].at[0, 0], tile_ref.at[k, n], sems.at[k, n]).wait()
        for n in range(slots):
            product = lax.dot_general(
                left,
                tile_ref[k, n],
                (((1,), (0 if by_rows else 1,)), ((), ())),
                preferred_element_type=jnp.float32,
            ).astype(jnp.bfloat16)
            places = jnp.where(lane == k * slots + n, targets[k][n], places)
            for q in range(blocks):
                product_ref[q, k * slots + n] = product[q * rows : (q + 1) * rows]
    places = places.astype(jnp.float32).astype(jnp.bfloat16)
    me = a if by_rows else b
    for k in range(blocks):
        send_refs[k][pl.ds(0, slots * slots)] = product_ref[me ^ k]
        send_refs[k][slots * slots] = places


def product_one(by_rows, index, lefts, parts, blocks, height):
    slots, tile = parts[0].shape[1:3]
    rows = height // blocks
    message = jax.ShapeDtypeStruct((slots * slots + 1, rows, tile), jnp.bfloat16)
    return pl.pallas_call(
        functools.partial(product_one_kernel, by_rows, len(lefts), len(parts)),
        out_shape=[message] * blocks,
        in_specs=[pl.BlockSpec(memory_space=SMEM)]
        + [pl.BlockSpec(memory_space=VMEM)] * len(lefts)
        + [pl.BlockSpec(memory_space=pltpu.HBM)] * len(parts),
        out_specs=[pl.BlockSpec(memory_space=VMEM)] * blocks,
        scratch_shapes=[
            pltpu.VMEM(lefts[0].shape, jnp.bfloat16),
            pltpu.VMEM((slots, slots, tile, tile), jnp.bfloat16),
            pltpu.VMEM((blocks, slots * slots, rows, tile), jnp.bfloat16),
            pltpu.SemaphoreType.DMA((slots, slots)),
        ],
        compiler_params=limit(50),
        cost_estimate=pl.CostEstimate(flops=12_000_000, bytes_accessed=4_000_000, transcendentals=0),
        name="one_rows" if by_rows else "one_columns",
    )(index, *lefts, *parts)


def merge_kernel(*refs):
    sources = len(refs) - 5
    message_refs, (out_ref, acc_ref, vector_ref, place_ref, sem) = refs[:sources], refs[sources:]
    count = message_refs[0].shape[0] - 1
    lines = [ref[count].astype(jnp.float32)[0:1] for ref in message_refs]
    lines += [jnp.zeros_like(lines[0])] * (8 - sources)
    vector_ref[...] = jnp.concatenate(lines, axis=0).astype(jnp.int32)
    copy = pltpu.make_async_copy(vector_ref, place_ref, sem)
    copy.start()
    acc_ref[...] = jnp.zeros_like(acc_ref)
    copy.wait()
    for e in range(count):
        for s in range(sources):
            acc_ref[place_ref[s, e]] += message_refs[s][e].astype(jnp.float32)
    out_ref[...] = acc_ref[...].astype(jnp.bfloat16)


def merge(messages, slab):
    _, rows, tile = messages[0].shape
    return pl.pallas_call(
        merge_kernel,
        out_shape=jax.ShapeDtypeStruct((slab, rows, tile), jnp.bfloat16),
        in_specs=[pl.BlockSpec(memory_space=VMEM)] * len(messages),
        out_specs=pl.BlockSpec(memory_space=VMEM),
        scratch_shapes=[
            pltpu.VMEM((slab, rows, tile), jnp.float32),
            pltpu.VMEM((8, 128), jnp.int32),
            pltpu.SMEM((8, 128), jnp.int32),
            pltpu.SemaphoreType.DMA,
        ],
        compiler_params=limit(8),
        cost_estimate=pl.CostEstimate(flops=4_000_000, bytes_accessed=1_000_000, transcendentals=0),
        name="merge",
    )(*messages)


def product_two_kernel(by_rows, here, blocks, index_ref, slab_ref, *refs):
    round_refs, refs = refs[:blocks], refs[blocks:]
    send_refs, (left_ref,) = refs[:blocks], refs[blocks:]
    g, a, b = lax.axis_index("gx"), lax.axis_index("gy"), lax.axis_index("gz")
    slab, slots = slab_ref.shape[:2]
    rows = left_ref.shape[2]
    for k in range(blocks):
        left_ref[k if by_rows else a ^ b ^ k] = round_refs[k][...]
    extra = jnp.where(a == b, 3.0, 0.0).astype(jnp.float32)

    def left_of(p):
        return jnp.concatenate([left_ref[m, p] for m in range(blocks)], axis=0)

    def one(q, lefts, tiles, same):
        summed = None
        for n in range(0, slots, 2):
            left = jnp.concatenate([left_of(p) for p in lefts[n : n + 2]], axis=1)
            pair = jnp.concatenate(tiles[n : n + 2], axis=1 if by_rows else 0)
            if by_rows:
                first, second, contract = pair, left, 1
            else:
                first, second, contract = left, pair, 0
            product = lax.dot_general(
                first,
                second,
                (((1,), (contract,)), ((), ())),
                preferred_element_type=jnp.float32,
            )
            summed = product if summed is None else summed + product
        summed = summed.T if by_rows else summed
        for m in range(blocks):
            value = extra * left_ref[m, same].astype(jnp.float32) - 2.0 * summed[m * rows : (m + 1) * rows]
            send_refs[m][q] = value.astype(jnp.bfloat16)

    unroll = math.gcd(UNROLL, slab)

    @pl.loop(0, slab, step=unroll)
    def _(first):
        for u in range(unroll):
            q = first + u
            entries = [index_ref[q, n] if by_rows else index_ref[n, q] for n in range(slots)]
            if by_rows:
                tiles = [slab_ref[q, j] for j in range(slots)]
                one(q, entries, tiles, lax.rem(q + here * g, slab))
            else:
                lefts = [entry >> 3 for entry in entries]
                tiles = [slab_ref[entry >> 3, entry & 7] for entry in entries]
                one(q, lefts, tiles, lax.rem(q + slab - here * g, slab))


def product_two(by_rows, index, rounded, tiles, here):
    slab, _, tile = tiles.shape[:3]
    blocks = len(rounded)
    rows = rounded[0].shape[1]
    message = jax.ShapeDtypeStruct((slab, rows, tile), jnp.bfloat16)
    return pl.pallas_call(
        functools.partial(product_two_kernel, by_rows, here, blocks),
        out_shape=[message] * blocks,
        in_specs=[pl.BlockSpec(memory_space=SMEM)]
        + [pl.BlockSpec(memory_space=VMEM)] * (1 + blocks),
        out_specs=[pl.BlockSpec(memory_space=VMEM)] * blocks,
        scratch_shapes=[pltpu.VMEM((blocks, slab, rows, tile), jnp.bfloat16)],
        compiler_params=limit(20),
        cost_estimate=pl.CostEstimate(flops=30_000_000, bytes_accessed=12_000_000, transcendentals=0),
        name="two_rows" if by_rows else "two_columns",
    )(index, tiles, *rounded)


def finish_kernel(here, half, *refs):
    out_ref, sum_ref, sem = refs[-3:]
    parts = refs[half:-3]
    slab, rows, tile = parts[0].shape
    turn = here * lax.axis_index("gx") if half else 0

    @pl.loop(0, slab, unroll=8)
    def _(y):
        q = lax.rem(y + slab - turn, slab) if half else y
        summed = parts[0][q].astype(jnp.float32)
        for ref in parts[1:]:
            summed = summed + ref[q].astype(jnp.float32)
        sum_ref[:, pl.ds(pl.multiple_of(y * tile, tile), tile)] = summed

    copy = pltpu.make_async_copy(sum_ref, out_ref.at[pl.ds(half * rows, rows)], sem)
    copy.start()
    copy.wait()


def finish(parts, here, before=None):
    slab, rows, tile = parts[0].shape
    ahead = () if before is None else (before,)
    return pl.pallas_call(
        functools.partial(finish_kernel, here, len(ahead)),
        out_shape=jax.ShapeDtypeStruct((2 * rows, slab * tile), jnp.float32),
        in_specs=[pl.BlockSpec(memory_space=pltpu.HBM)] * len(ahead)
        + [pl.BlockSpec(memory_space=VMEM)] * len(parts),
        out_specs=pl.BlockSpec(memory_space=pltpu.HBM),
        scratch_shapes=[pltpu.VMEM((rows, slab * tile), jnp.float32), pltpu.SemaphoreType.DMA],
        input_output_aliases={0: 0} if ahead else {},
        compiler_params=limit(50),
        cost_estimate=pl.CostEstimate(flops=1_000_000, bytes_accessed=1_000_000, transcendentals=0),
        name="finish",
    )(*ahead, *parts)


def local(block_values, block_cols):
    tiles_here = block_values[0, :, 0]
    columns_here = block_cols[0, :, 0]
    here, _, tile, _ = tiles_here.shape
    parts = lax.axis_size("gx")
    size = lax.axis_size("gy")
    blocks = WIN * tile // size
    rows = blocks // 2
    height = rows * size

    pay_a, pay_b = payloads(tiles_here, columns_here, height)
    both = ("gy", "gz")
    shifts = [[((i + t) % parts, i) for i in range(parts)] for t in range(1, parts)]
    others = [lax.ppermute(columns_here, "gx", s) for s in shifts]
    moved = [lax.ppermute(tiles_here, "gx", s) for s in shifts]
    left_b = []
    for k in range(size):
        left_b.append(lax.ppermute(pay_b, both, [(a, a * size + (a ^ k)) for a in range(size)]))
    left_a = [pay_a]
    for k in range(1, size):
        left_a.append(lax.ppermute(pay_a, "gy", [(0, k)]))
    columns = jnp.concatenate([columns_here] + others, axis=0)
    inverse = invert(columns)
    pieces = [tiles_here] + moved

    def scatter(sends, axis):
        received = [sends[0]]
        for k in range(1, size):
            received.append(lax.ppermute(sends[k], axis, swaps(size, k)))
        return received

    def spread(own, axis):
        return scatter([own] * size, axis)

    sends_a = product_one(False, inverse, left_a, pieces, size, height)
    parts_a = scatter(sends_a, "gz")
    _, left_b = lax.optimization_barrier((sends_a[0], left_b))
    sends_b = product_one(True, columns, left_b, pieces, size, height)
    parts_b = scatter(sends_b, "gy")
    tiles = assemble(pieces)
    own_b = merge(parts_b, here * parts)
    own_a = merge(parts_a, here * parts)
    rounded_b = spread(own_b, "gy")
    rounded_a = spread(own_a, "gz")
    out_b = product_two(True, columns, rounded_b, tiles, here)
    crossed = scatter(out_b, "gy")
    picked = pick(crossed)
    got_b = scatter(picked, "gz")
    out_a = product_two(False, inverse, rounded_a, tiles, here)
    got_a = scatter(out_a, "gy")
    begun = finish(got_a, here)
    return finish(got_b, here, begun)


def solution(mesh):
    in_specs = (P("gy", "gx", "gz", None, None, None), P("gy", "gx", "gz", None))
    out_specs = P(("gx", "gy"), "gz")
    return jax.shard_map(local, mesh=mesh, in_specs=in_specs, out_specs=out_specs, check_vma=False)
```
